16 devices in a mesh: dp: 2 (over z), fsdp: 8 (over y, x, core).
Axes of the slice: x: 2, y: 2, z: 2, core: 2. Of those that a mesh axis runs over, the one named last changes fastest.
Arguments:
- tokens: bfloat16 [32, 256, 2048], P(('dp', 'fsdp')), parts along dimension 0
- w_query: bfloat16 [2, 2048, 2048], P(None, 'fsdp')
- w_key: bfloat16 [2, 2048, 2048], P(None, 'fsdp')
- w_value: bfloat16 [2, 2048, 2048], P(None, 'fsdp')
- w_out: bfloat16 [2, 2048, 2048], P(None, 'fsdp')
- w_gate: bfloat16 [2, 2048, 8192], P(None, 'fsdp')
- w_up: bfloat16 [2, 2048, 8192], P(None, 'fsdp')
- w_down: bfloat16 [2, 8192, 2048], P(None, 'fsdp')
- g_query: bfloat16 [2, 2048], P(None, 'fsdp')
- g_key: bfloat16 [2, 2048], P(None, 'fsdp')
- g_attn: bfloat16 [2, 2048], P(None, 'fsdp')
- g_mlp: bfloat16 [2, 2048], P(None, 'fsdp')
Outputs:
- output: bfloat16 [32, 256, 2048], P(('dp', 'fsdp')), parts along dimension 0
There are 2 independent parts. The reference program is written for one: setup_inputs(seed, part) draws one part's arguments, and reference() takes and returns one part's arrays. A program takes and returns all parts, laid end to end along the dimension named above; an argument that names none is the same for every part.
All inputs are finite; a program needn't handle non-finite values.
Results may differ from the reference program's by a relative error of at most 0.02.
Values are sent between devices in bfloat16 or wider.
A program may use at most 1 GiB of HBM per device.

```python
import jax
import jax.numpy as jnp
from jax import lax

D = 2048
FF = 8192
HEADS = 16
SEQ = 256
BATCH = 16
LAYERS = 2
HEAD = D // HEADS
Q_BLOCK = min(SEQ, 256)
EPS = 1e-6
THETA = 500000.0


def setup_inputs(seed: int = 0, part: int = 0) -> dict:
    key_main = jax.random.key(seed)
    key_tok = jax.random.fold_in(jax.random.key(seed + 1), part)
    key_list = jax.random.split(key_main, 11)

    def make_weight(key_w, n_rows, n_cols):
        draw = jax.random.normal(key_w, (LAYERS, n_rows, n_cols), jnp.float32)
        return (draw * n_rows ** -0.5).astype(jnp.bfloat16)

    def make_gain(key_g):
        key_mag, key_sign = jax.random.split(key_g)
        magnitude = jax.random.uniform(key_mag, (LAYERS, D), jnp.float32, 0.5, 1.5)
        sign_vec = jnp.where(jax.random.bernoulli(key_sign, 0.5, (LAYERS, D)), 1.0, -1.0)
        return (magnitude * sign_vec).astype(jnp.bfloat16)

    tokens = jax.random.normal(key_tok, (BATCH, SEQ, D), jnp.float32).astype(jnp.bfloat16)
    return dict(
        tokens=tokens,
        w_query=make_weight(key_list[0], D, D),
        w_key=make_weight(key_list[1], D, D),
        w_value=make_weight(key_list[2], D, D),
        w_out=make_weight(key_list[3], D, D),
        w_gate=make_weight(key_list[4], D, FF),
        w_up=make_weight(key_list[5], D, FF),
        w_down=make_weight(key_list[6], FF, D),
        g_query=make_gain(key_list[7]),
        g_key=make_gain(key_list[8]),
        g_attn=make_gain(key_list[9]),
        g_mlp=make_gain(key_list[10]),
    )


def rms_norm(values, gain_vec):
    mean_sq = jnp.mean(values * values, axis=-1, keepdims=True)
    return values * lax.rsqrt(mean_sq + EPS) * gain_vec.astype(jnp.float32)


def rope_tables():
    positions = jnp.arange(SEQ, dtype=jnp.float32)
    inv_freq = THETA ** (-2.0 * jnp.arange(HEAD // 2, dtype=jnp.float32) / HEAD)
    angles = positions[:, None] * inv_freq[None, :]
    return jnp.cos(angles), jnp.sin(angles)


def apply_rope(values, cos_tab, sin_tab):
    half_dim = values.shape[-1] // 2
    first = values[..., :half_dim]
    second = values[..., half_dim:]
    cos_b = cos_tab[:, None, :]
    sin_b = sin_tab[:, None, :]
    return jnp.concatenate([first * cos_b - second * sin_b, second * cos_b + first * sin_b], axis=-1)


def matmul_bf16(left, right):
    return jnp.dot(left, right, preferred_element_type=jnp.float32).astype(jnp.bfloat16)


def layer_seq(seq_x, layer_w, cos_tab, sin_tab):
    w_query, w_key, w_value, w_out, w_gate, w_up, w_down, g_query, g_key, g_attn, g_mlp = layer_w
    q_lin = matmul_bf16(seq_x, w_query)
    k_lin = matmul_bf16(seq_x, w_key)
    v_lin = matmul_bf16(seq_x, w_value)
    q_rot = apply_rope(rms_norm(q_lin.astype(jnp.float32), g_query).reshape(SEQ, HEADS, HEAD), cos_tab, sin_tab).astype(jnp.bfloat16)
    k_rot = apply_rope(rms_norm(k_lin.astype(jnp.float32), g_key).reshape(SEQ, HEADS, HEAD), cos_tab, sin_tab).astype(jnp.bfloat16)
    k_full = k_rot.astype(jnp.float32)
    v_full = v_lin.reshape(SEQ, HEADS, HEAD).astype(jnp.float32)
    q_blocks = q_rot.reshape(SEQ // Q_BLOCK, Q_BLOCK, HEADS, HEAD)
    key_pos = jnp.arange(SEQ)

    def attend(block_in):
        q_blk, block_idx = block_in
        scores = jnp.einsum('qhd,khd->hqk', q_blk.astype(jnp.float32), k_full) * HEAD ** -0.5
        q_pos = block_idx * Q_BLOCK + jnp.arange(Q_BLOCK)
        causal = q_pos[:, None] >= key_pos[None, :]
        scores = jnp.where(causal[None, :, :], scores, -jnp.inf)
        probs = jax.nn.softmax(scores, axis=-1).astype(jnp.bfloat16).astype(jnp.float32)
        return jnp.einsum('hqk,khd->qhd', probs, v_full).astype(jnp.bfloat16)

    attn_blocks = lax.map(attend, (q_blocks, jnp.arange(SEQ // Q_BLOCK)))
    a_lin = matmul_bf16(attn_blocks.reshape(SEQ, D), w_out)
    hidden = (seq_x.astype(jnp.float32) + rms_norm(a_lin.astype(jnp.float32), g_attn)).astype(jnp.bfloat16)
    gate_proj = matmul_bf16(hidden, w_gate)
    up_proj = matmul_bf16(hidden, w_up)
    gated = (jax.nn.silu(gate_proj.astype(jnp.float32)) * up_proj.astype(jnp.float32)).astype(jnp.bfloat16)
    down_proj = matmul_bf16(gated, w_down)
    return (hidden.astype(jnp.float32) + rms_norm(down_proj.astype(jnp.float32), g_mlp)).astype(jnp.bfloat16)


def reference(tokens, w_query, w_key, w_value, w_out, w_gate, w_up, w_down, g_query, g_key, g_attn, g_mlp):
    cos_tab, sin_tab = rope_tables()

    def one_layer(carry, layer_w):
        out_seq = lax.map(lambda seq_x: layer_seq(seq_x, layer_w, cos_tab, sin_tab), carry)
        return out_seq, None

    result, _ = lax.scan(one_layer, tokens, (w_query, w_key, w_value, w_out, w_gate, w_up, w_down, g_query, g_key, g_attn, g_mlp))
    return result
```

```python
import functools

import jax
import jax.numpy as jnp
import numpy as np
from jax import lax
from jax.experimental import pallas as pl
from jax.experimental.pallas import tpu as pltpu
from jax.sharding import PartitionSpec as P

HEAD_DIM = 128
EPS = 1e-6
THETA = 500000.0
SEQ = 256
D = 2048
ROWS = 512
N_BLK = 8
BLK = 256
PER_LAYER = 16
N_CHUNK = 32
PLANE = 176
ZP = 80
VIA_X = 80
VIA_Y = PLANE - VIA_X
A_OWN, A_FIRST, A_DIAG, A_PAIR = 6, 4, 3, 1
SLOTS = 4
TILE = 512
N_TILE = D // TILE
RB = 32

K_X, K_Y, K_P0, K_DX, K_DY, K_ZX, K_ZY, K_ZD, K_P1, K_P2, K_P3 = range(11)
N_KIND = 11
KIND_ROWS = (PLANE, PLANE, BLK, VIA_X, VIA_Y, ZP, ZP, ZP, BLK, BLK, BLK)


def rope_tables():
    pos = np.arange(SEQ, dtype=np.float64)
    inv = THETA ** (-2.0 * np.arange(HEAD_DIM // 2, dtype=np.float64) / HEAD_DIM)
    ang = pos[:, None] * inv[None, :]
    cos, sin = np.cos(ang), np.sin(ang)
    return (np.concatenate([cos, cos], 1).astype(np.float32), np.concatenate([-sin, sin], 1).astype(np.float32))


def kernel(x_hbm, cos_ref, sin_ref, gain_ref, wq, wk, wv, wo, wg, wu, wd, out_hbm, full, act, acc, wt, gains, send_sem, recv_sem, wt_sem, gs_sem, gr_sem, io_sem):
    zz = lax.axis_index('dp')
    me = lax.axis_index('fsdp')
    cc = me % 2
    xx = (me // 2) % 2
    yy = me // 4

    def at(y, x, c):
        return y * 4 + x * 2 + c

    f_p = at(yy, xx, 1 - cc)
    f_x = at(yy, 1 - xx, cc)
    f_y = at(1 - yy, xx, cc)
    f_d = at(1 - yy, 1 - xx, cc)
    dev_p, dev_x, dev_y, dev_z = (zz, f_p), (zz, f_x), (zz, f_y), (1 - zz, me)

    x_copy = pltpu.make_async_copy(x_hbm, act.at[0], io_sem)
    x_copy.start()

    barrier = pltpu.get_barrier_semaphore()
    for k in range(1, N_BLK):
        pl.semaphore_signal(barrier, inc=1, device_id=(zz, (me + k) % N_BLK), device_id_type=pl.DeviceIdType.MESH)
    pl.semaphore_signal(barrier, inc=1, device_id=dev_z, device_id_type=pl.DeviceIdType.MESH)
    pl.semaphore_wait(barrier, N_BLK)

    gain_copies = []
    for k in range(1, N_BLK):
        cp = pltpu.make_async_remote_copy(gain_ref, gains.at[me], gs_sem.at[k], gr_sem.at[k], device_id=(zz, (me + k) % N_BLK), device_id_type=pl.DeviceIdType.MESH)
        cp.start()
        gain_copies.append(cp)

    def m16(v):
        return pl.multiple_of(v, 16)

    off_plane = m16(ZP * zz)
    off_dx = m16(ZP * zz)
    off_dy = m16(ZP * zz + VIA_X)
    off_z = m16(PLANE * zz)

    def own(i, fn):
        la = i // PER_LAYER
        t = i % PER_LAYER
        g = (t - 4) // 2
        for k, w in enumerate((wq, wk, wv, wo)):
            pl.when(t == k)(functools.partial(fn, w.at[la]))
        mid = (t >= 4) & (t < 12)
        cols = pl.ds(pl.multiple_of(g * D, D), D)

        @pl.when(mid & (t % 2 == 0))
        def _():
            fn(wg.at[la, :, cols])

        @pl.when(mid & (t % 2 == 1))
        def _():
            fn(wu.at[la, :, cols])

        @pl.when(t >= 12)
        def _():
            fn(wd.at[la, pl.ds(pl.multiple_of((t - 12) * BLK, BLK), BLK), :])

    def remote(kind, i, src, dst, dev):
        return pltpu.make_async_remote_copy(src, dst, send_sem.at[kind, i % SLOTS], recv_sem.at[kind, i], device_id=dev, device_id_type=pl.DeviceIdType.MESH)

    def drain(kind, i):
        piece = full.at[0, 0, pl.ds(0, KIND_ROWS[kind]), :]
        remote(kind, i, piece, piece, dev_p).wait_send()

    def arrived(kind, i):
        piece = full.at[0, 0, pl.ds(0, KIND_ROWS[kind]), :]
        remote(kind, i, piece, piece, dev_p).wait_recv()

    def push(kind, i, blk, off, dev):
        pl.when(i >= SLOTS)(functools.partial(drain, kind, i - SLOTS))
        piece = full.at[i, blk, pl.ds(off, KIND_ROWS[kind]), :]
        remote(kind, i, piece, piece, dev).start()

    def stage_own(i):
        for kind in (K_X, K_Y, K_P0):
            pl.when(i >= SLOTS)(functools.partial(drain, kind, i - SLOTS))

        def go(src):
            part = pl.ds(off_plane, PLANE)
            remote(K_X, i, src.at[part, :], full.at[i, me, part, :], dev_x).start()
            remote(K_Y, i, src.at[part, :], full.at[i, me, part, :], dev_y).start()
            remote(K_P0, i, src, full.at[i, me], dev_p).start()

        own(i, go)

    def stage_first(i):
        arrived(K_X, i)
        push(K_ZX, i, f_x, off_z, dev_z)
        push(K_DY, i, f_x, off_dy, dev_y)
        arrived(K_Y, i)
        push(K_ZY, i, f_y, off_z, dev_z)
        push(K_DX, i, f_y, off_dx, dev_x)

    def stage_diag(i):
        arrived(K_DX, i)
        arrived(K_DY, i)
        push(K_ZD, i, f_d, off_z, dev_z)

    def stage_pair(i):
        arrived(K_ZX, i)
        push(K_P1, i, f_x, 0, dev_p)
        arrived(K_ZY, i)
        push(K_P2, i, f_y, 0, dev_p)
        arrived(K_ZD, i)
        push(K_P3, i, f_d, 0, dev_p)

    def load_tile(i, n):
        slot = n % 2
        cols = pl.ds(n * TILE, TILE)

        def own_block(src):
            pltpu.make_async_copy(src.at[:, cols], wt.at[slot, me], wt_sem.at[slot]).start()

        own(i, own_block)
        for k in range(1, N_BLK):
            b = (me + k) % N_BLK
            pltpu.make_async_copy(full.at[i, b, :, cols], wt.at[slot, b], wt_sem.at[slot]).start()

    def wait_tile(n):
        slot = n % 2
        pltpu.make_async_copy(full.at[0, :, :, pl.ds(0, TILE)], wt.at[slot], wt_sem.at[slot]).wait()

    def gain_row(la, k):
        return jnp.concatenate([gains[f, pl.ds(la * 4 + k, 1), :] for f in range(N_BLK)], axis=1)

    def normed(r0, gain):
        a = acc[pl.ds(r0, RB), :].astype(jnp.bfloat16).astype(jnp.float32)
        ms = jnp.mean(a * a, axis=-1, keepdims=True)
        return a * lax.rsqrt(ms + EPS) * gain

    def rows(body):
        def step(r, carry):
            body(pl.multiple_of(r * RB, RB))
            return carry

        lax.fori_loop(0, ROWS // RB, step, 0)

    def norm_rope(la, k, dst):
        gain = gain_row(la, k)

        def body(r0):
            v = normed(r0, gain)
            p0 = pl.multiple_of(r0 % SEQ, RB)
            c = cos_ref[pl.ds(p0, RB), :]
            s = sin_ref[pl.ds(p0, RB), :]
            for h in range(D // HEAD_DIM):
                part = v[:, h * HEAD_DIM:(h + 1) * HEAD_DIM]
                turned = pltpu.roll(part, HEAD_DIM // 2, 1)
                act[dst, pl.ds(r0, RB), h * HEAD_DIM:(h + 1) * HEAD_DIM] = (part * c + turned * s).astype(jnp.bfloat16)

        rows(body)

    def attention():
        row = lax.broadcasted_iota(jnp.int32, (SEQ, SEQ), 0)
        col = lax.broadcasted_iota(jnp.int32, (SEQ, SEQ), 1)
        causal = row >= col

        def step(h, carry):
            lanes = pl.ds(pl.multiple_of(h * HEAD_DIM, HEAD_DIM), HEAD_DIM)
            for b in range(ROWS // SEQ):
                sq = pl.ds(b * SEQ, SEQ)
                q, k, v = act[1, sq, lanes], act[2, sq, lanes], act[3, sq, lanes]
                s = lax.dot_general(q, k, (((1,), (1,)), ((), ())), preferred_element_type=jnp.float32) * (HEAD_DIM ** -0.5)
                s = jnp.where(causal, s, -jnp.inf)
                e = jnp.exp(s - jnp.max(s, axis=-1, keepdims=True))
                p = (e / jnp.sum(e, axis=-1, keepdims=True)).astype(jnp.bfloat16)
                act[1, sq, lanes] = jnp.dot(p, v, preferred_element_type=jnp.float32).astype(jnp.bfloat16)
            return carry

        lax.fori_loop(0, D // HEAD_DIM, step, 0)

    def residual(la, k, src, dst):
        gain = gain_row(la, k)

        def body(r0):
            rr = pl.ds(r0, RB)
            act[dst, rr, :] = (act[src, rr, :].astype(jnp.float32) + normed(r0, gain)).astype(jnp.bfloat16)

        rows(body)

    def compute(i):
        la = i // PER_LAYER
        t = i % PER_LAYER
        lhs = jnp.where(t < 3, 0, jnp.where(t == 3, 1, jnp.where(t < 12, 4, t - 7)))
        keep = t > 12
        load_tile(i, 0)
        for n in range(N_TILE):
            if n + 1 < N_TILE:
                load_tile(i, n + 1)
            wait_tile(n)
            cols = slice(n * TILE, (n + 1) * TILE)
            prod = jnp.dot(act[lhs], wt[n % 2].reshape(D, TILE), preferred_element_type=jnp.float32)
            acc[:, cols] = jnp.where(keep, acc[:, cols], 0.0) + prod

        @pl.when(i == 0)
        def _():
            for cp in gain_copies:
                cp.wait()
            gains[pl.ds(me, 1)] = gain_ref[...][None]

        @pl.when(t == 0)
        def _():
            norm_rope(la, 0, 1)

        @pl.when(t == 1)
        def _():
            norm_rope(la, 1, 2)

        @pl.when(t == 2)
        def _():
            def body(r0):
                act[3, pl.ds(r0, RB), :] = acc[pl.ds(r0, RB), :].astype(jnp.bfloat16)

            rows(body)
            attention()

        @pl.when(t == 3)
        def _():
            residual(la, 2, 0, 4)

        mid = (t >= 4) & (t < 12)

        @pl.when(mid & (t % 2 == 0))
        def _():
            def body(r0):
                act[2, pl.ds(r0, RB), :] = acc[pl.ds(r0, RB), :].astype(jnp.bfloat16)

            rows(body)

        @pl.when(mid & (t % 2 == 1))
        def _():
            g = (t - 4) // 2

            def body(r0):
                rr = pl.ds(r0, RB)
                for c in range(N_BLK):
                    cols = slice(c * BLK, (c + 1) * BLK)
                    gate = act[2, rr, cols].astype(jnp.float32)
                    up = acc[rr, cols].astype(jnp.bfloat16).astype(jnp.float32)
                    val = (jax.nn.silu(gate) * up).astype(jnp.bfloat16)
                    lanes = pl.ds(pl.multiple_of((2 * g + c // 4) * BLK, BLK), BLK)
                    act[5 + c % 4, rr, lanes] = val

            rows(body)

        @pl.when(t == 15)
        def _():
            residual(la, 3, 4, 0)

    x_copy.wait()

    def step(it, carry):
        i = it - A_OWN
        for ahead, stage in ((A_OWN, stage_own), (A_FIRST, stage_first), (A_DIAG, stage_diag), (A_PAIR, stage_pair)):
            j = i + ahead
            pl.when((j >= 0) & (j < N_CHUNK))(functools.partial(stage, j))

        @pl.when(i >= 0)
        def _():
            for kind in (K_P0, K_P1, K_P2, K_P3):
                arrived(kind, i)
            compute(i)

        return carry

    lax.fori_loop(0, N_CHUNK + A_OWN, step, 0)

    for kind in range(N_KIND):
        for i in range(N_CHUNK - SLOTS, N_CHUNK):
            drain(kind, i)
    out_copy = pltpu.make_async_copy(act.at[0], out_hbm, io_sem)
    out_copy.start()
    out_copy.wait()


def solution(mesh):
    cos_np, sin_np = rope_tables()
    hbm = pl.BlockSpec(memory_space=pl.ANY)
    vmem = pl.BlockSpec(memory_space=pltpu.VMEM)

    def local_fn(tokens, weights, gain_vecs):
        gains = jnp.stack(gain_vecs, axis=1).reshape(8, BLK).astype(jnp.float32)
        flat = tokens.reshape(ROWS, D)
        out, _ = pl.pallas_call(
            kernel,
            out_shape=(jax.ShapeDtypeStruct((ROWS, D), jnp.bfloat16), jax.ShapeDtypeStruct((N_CHUNK, N_BLK, BLK, D), jnp.bfloat16)),
            in_specs=[hbm, vmem, vmem, vmem] + [hbm] * 7,
            out_specs=(hbm, hbm),
            scratch_shapes=[
                pltpu.VMEM((9, ROWS, D), jnp.bfloat16),
                pltpu.VMEM((ROWS, D), jnp.float32),
                pltpu.VMEM((2, N_BLK, BLK, TILE), jnp.bfloat16),
                pltpu.VMEM((N_BLK, 8, BLK), jnp.float32),
                pltpu.SemaphoreType.DMA((N_KIND, SLOTS)),
                pltpu.SemaphoreType.DMA((N_KIND, N_CHUNK)),
                pltpu.SemaphoreType.DMA((2,)),
                pltpu.SemaphoreType.DMA((N_BLK,)),
                pltpu.SemaphoreType.DMA((N_BLK,)),
                pltpu.SemaphoreType.DMA,
            ],
            compiler_params=pltpu.CompilerParams(collective_id=0, has_side_effects=True, vmem_limit_bytes=60 * 1024 * 1024),
        )(flat, jnp.asarray(cos_np), jnp.asarray(sin_np), gains, *weights)
        return out.reshape(tokens.shape)

    mapped = jax.shard_map(local_fn, mesh=mesh, in_specs=(P(('dp', 'fsdp')), P(None, 'fsdp'), P(None, 'fsdp')), out_specs=P(('dp', 'fsdp')), check_vma=False)

    def run(tokens, w_query, w_key, w_value, w_out, w_gate, w_up, w_down, g_query, g_key, g_attn, g_mlp):
        return mapped(tokens, (w_query, w_key, w_value, w_out, w_gate, w_up, w_down), (g_query, g_key, g_attn, g_mlp))

    return run
```

```python
import functools

import jax
import jax.numpy as jnp
import numpy as np
from jax import lax
from jax.experimental import pallas as pl
from jax.experimental.pallas import tpu as pltpu
from jax.sharding import PartitionSpec as P

HEAD_DIM = 128
EPS = 1e-6
THETA = 500000.0
SEQ = 256
D = 2048
ROWS = 512
N_BLK = 8
BLK = 256
TILE = 512
N_TILE = D // TILE
RB = 32
MESH = pl.DeviceIdType.MESH

UNIT = 22.5 / 256
LAT = 2.5
PAIR = 4.0
FLOW = {'A': (160, 128, 80, 48, 0), 'B': (128, 192, 0, 128, 0), 'H': (256, 128, 0, 128, 160), 'G': (224, 176, 0, 128, 192)}
ITEMS = ['A'] * 4 + ['H'] * 4 + ['B'] * 4 + ['G'] * 3 + ['B'] * 3
N_H = (4, 3)
BACKLOG = 18.0
COST = {'mm': 5.0, 'at': 7.0, 'h': 12.0, 'wgu': 9.0, 'wd': 9.0, 'fin': 3.0}


def slots(nh=(4, 3)):
    out = []
    for k in range(3):
        out.append(('mm', k, 0, k, 2))
    base = 4
    attn = (0, 4 + nh[0])
    for la in range(2):
        for s in range(2):
            if la:
                for k in range(3):
                    out.append(('mm', attn[1] + k, 1, k, s))
            for q in range(2):
                out.append(('at', 0, la, q, s))
            out.append(('mm', attn[la] + 3, la, 3, s))
        h0 = attn[la] + 4
        if la == 0:
            for j in range(nh[0]):
                for s in range(2):
                    out.append(('h', h0 + j, 0, j, s))
        else:
            for s in range(2):
                for j in range(nh[1]):
                    out.append(('h', h0 + j, 1, j, s))
            w0 = h0 + nh[1]
            if nh[1] < 4:
                out.append(('wgu', w0, 1, 0, 2))
                out.append(('wgu', w0 + 1, 1, 1, 2))
                out.append(('wd', w0 + 2, 1, 4, 2))
        for s in range(2):
            out.append(('fin', 0, la, 0, s))
    return out


def schedule(thr=20.0, nh=(4, 3)):
    sl = slots(nh)
    t = 0.0
    free = dict(x=0.0, y=0.0, z=0.0, p=0.0)
    arr = {}
    prog = []
    busy = dict(x=0.0, y=0.0, z=0.0, p=0.0)

    def send(link, dur, key):
        s = max(free[link], t)
        free[link] = s + dur
        busy[link] += dur
        arr[key] = free[link] + LAT

    xq = [i for i in range(len(ITEMS))]
    yq = []
    for i, f in enumerate(ITEMS):
        yq.append(('oy', i))
        if f in 'HG':
            yq.append(('on', i))
    pend = []
    for i, f in enumerate(ITEMS):
        px, py, dx, dy, pn = FLOW[f]
        pend.append((('fx', i), [('X', i)]))
        pend.append((('fy', i), [('Y', i)]))
        pend.append((('fd', i), ([('DX', i)] if dx else []) + [('DY', i)]))
        if px < 256:
            pend.append((('px', i), [('X', i), ('ZX', i)]))
        pend.append((('py', i), [('Y', i), ('ZY', i)]))
        pend.append((('pd', i), ([('DX', i)] if dx else []) + [('DY', i), ('ZD', i)]))
        if pn:
            pend.append((('fn', i), [('N', i)]))
            pend.append((('pn', i), [('N', i), ('ZN', i)]))

    def run(op):
        if op[0] in ('ag', 'rs'):
            units, key = (1, 'H') if op[0] == 'ag' else (2, 'R')
            send('x', units * 22.5, (key,) + op[1:])
            prog.append(op)
            return
        kind, i = op
        px, py, dx, dy, pn = FLOW[ITEMS[i]]
        if kind == 'ox':
            send('x', px * UNIT, ('X', i))
        elif kind == 'oy':
            send('y', py * UNIT, ('Y', i))
            send('p', PAIR, ('P0', i))
        elif kind == 'on':
            send('y', pn * UNIT, ('N', i))
            send('p', PAIR, ('Q0', i))
        elif kind == 'fx':
            if px < 256:
                send('z', (256 - px) * UNIT, ('ZX', i))
            else:
                send('p', PAIR, ('P1', i))
            send('y', dy * UNIT, ('DY', i))
        elif kind == 'fy':
            send('z', (256 - py) * UNIT, ('ZY', i))
            if dx:
                send('x', dx * UNIT, ('DX', i))
        elif kind == 'fd':
            send('z', (256 - dx - dy) * UNIT, ('ZD', i))
        elif kind == 'fn':
            send('z', (256 - pn) * UNIT, ('ZN', i))
        elif kind in ('px', 'py', 'pd'):
            send('p', PAIR, (dict(px='P1', py='P2', pd='P3')[kind], i))
        elif kind == 'pn':
            send('p', PAIR, ('Q1', i))
        prog.append(op)

    def needs(s):
        ty, it, la, ex, hf = s
        n = []
        if ty in ('mm', 'h', 'wgu', 'wd'):
            n += [('P%d' % k, it) for k in range(4)]
        if ty == 'h':
            n += [('Q%d' % k, it) for k in range(2)]
            n.append(('H', la, hf))
        if ty == 'fin':
            n.append(('R', la, hf))
        return n

    def after(s):
        ty, it, la, ex, hf = s
        if ty == 'mm' and ex < 3:
            return [('fin', la - 1, 0, hf)] if la else []
        if ty == 'at':
            return [('mm', la, k, hf if la else 2) for k in range(3)]
        if ty == 'mm':
            return [('at', la, q, hf) for q in range(2)]
        if ty == 'h':
            return [('mm', la, 3, hf)] + ([('h', la, ex - 1, hf)] if ex else [])
        if ty == 'wgu':
            return [('mm', la, 3, 0), ('mm', la, 3, 1)]
        if ty == 'wd':
            return [('wgu', la, 0, 2), ('wgu', la, 1, 2)] + [('h', la, nh[1] - 1, q) for q in range(2)]
        return [('h', la, nh[la] - 1, hf)] + ([('wd', la, 4, 2)] if la and nh[1] < 4 else [])

    done = set()
    todo = list(range(len(sl)))
    while todo:
        again = True
        while again:
            again = False
            for op, ns in list(pend):
                if all(arr.get(x, 1e9) <= t for x in ns):
                    pend.remove((op, ns))
                    run(op)
                    again = True
            if xq and free['x'] - t < thr:
                run(('ox', xq.pop(0)))
                again = True
            if yq and free['y'] - t < thr:
                run(yq.pop(0))
                again = True
        pick = None
        ev = [arr[x] for op, n2 in pend for x in n2 if x in arr]
        for k in todo:
            s = sl[k]
            if not all(x in done for x in after(s)):
                continue
            ns = needs(s)
            if all(arr.get(x, 1e9) <= t for x in ns):
                pick = k
                break
            ev += [arr[x] for x in ns if x in arr]
        if pick is not None:
            s = sl[pick]
            todo.remove(pick)
            prog.append(('slot', pick))
            t += COST[s[0]] * (2 if s[0] == 'mm' and s[4] == 2 else 1)
            done.add((s[0], s[2], s[3], s[4]))
            if s[0] == 'mm' and s[3] == 3:
                run(('ag', s[2], s[4]))
            if s[0] == 'h' and s[3] == nh[s[2]] - 1:
                run(('rs', s[2], s[4]))
            continue
        if xq:
            ev.append(free['x'] - thr + 0.01)
        if yq:
            ev.append(free['y'] - thr + 0.01)
        t = min(e for e in ev if e > t)
    assert not pend and not xq and not yq
    return sl, prog, t


def plan():
    sl, prog, _ = schedule(BACKLOG, N_H)
    order, lists, cur, seen = [], [], [], set()
    for op in prog:
        if op[0] != 'slot':
            cur.append(op)
            continue
        s = sl[op[1]]
        ty, it, la, ex, hf = s
        need = []
        if ty in ('mm', 'h', 'wgu', 'wd'):
            need += [('P%d' % k, it) for k in range(4)]
        if ty == 'h':
            need += [('Q%d' % k, it) for k in range(2)] + [('H', la, hf)]
            if la == 1 and ex == 0:
                cur.append(('drain', ('R', 0, hf)))
        if ty == 'fin':
            need.append(('R', la, hf))
        for key in need:
            if key not in seen:
                seen.add(key)
                cur.append(('wait', key))
        order.append(s)
        lists.append(cur)
        cur = []
    assert not cur or all(op[0] in ('ag', 'rs') for op in cur)
    return order, lists


def copy_keys():
    keys = []
    for i, f in enumerate(ITEMS):
        px, py, dx, dy, pn = FLOW[f]
        rows = {'X': px, 'Y': py, 'P0': BLK, 'DX': dx, 'DY': dy, 'ZX': BLK - px, 'ZY': BLK - py, 'ZD': BLK - dx - dy, 'P1': BLK, 'P2': BLK, 'P3': BLK}
        if pn:
            rows.update({'N': pn, 'ZN': BLK - pn, 'Q0': BLK, 'Q1': BLK})
        keys += [((k, i), r) for k, r in rows.items() if r]
    for la in range(2):
        for s in range(2):
            keys += [(('H', la, s), BLK), (('R', la, s), 0)]
    return keys


KEYS = copy_keys()
SID = {k: n for n, (k, _) in enumerate(KEYS)}
KROWS = dict(KEYS)
H_ITEMS = [i for i, f in enumerate(ITEMS) if FLOW[f][4]]
ATTN0 = (0, 4 + N_H[0])
W_ITEM = 8 + N_H[0] + N_H[1]


def rope_tables():
    pos = np.arange(SEQ, dtype=np.float64)
    inv = THETA ** (-2.0 * np.arange(HEAD_DIM // 2, dtype=np.float64) / HEAD_DIM)
    ang = pos[:, None] * inv[None, :]
    cos, sin = np.cos(ang), np.sin(ang)
    return (np.concatenate([cos, cos], 1).astype(np.float32), np.concatenate([-sin, sin], 1).astype(np.float32))


def kernel(x_hbm, cos_ref, sin_ref, gain_ref, wq, wk, wv, wo, wg, wu, wd, out_hbm, full, full_n, act, h2, mj, acc, rs, wt, gains, send_sem, recv_sem, wt_sem, gs_sem, gr_sem, io_sem):
    zz = lax.axis_index('dp')
    me = lax.axis_index('fsdp')
    cc = me % 2
    xx = (me // 2) % 2
    yy = me // 4

    def at(y, x, c):
        return y * 4 + x * 2 + c

    f_p = at(yy, xx, 1 - cc)
    f_x = at(yy, 1 - xx, cc)
    f_y = at(1 - yy, xx, cc)
    f_d = at(1 - yy, 1 - xx, cc)
    n_me, n_y = yy * 2 + cc, (1 - yy) * 2 + cc
    dev_p, dev_x, dev_y, dev_z = (zz, f_p), (zz, f_x), (zz, f_y), (1 - zz, me)

    x_copy = pltpu.make_async_copy(x_hbm, act.at[0], io_sem)
    x_copy.start()

    barrier = pltpu.get_barrier_semaphore()
    for k in range(1, N_BLK):
        pl.semaphore_signal(barrier, inc=1, device_id=(zz, (me + k) % N_BLK), device_id_type=MESH)
    pl.semaphore_signal(barrier, inc=1, device_id=dev_z, device_id_type=MESH)
    pl.semaphore_wait(barrier, N_BLK)

    def m16(v):
        return pl.multiple_of(v, 16)

    def m256(v):
        return pl.multiple_of(v, 256)

    def remote(key, src, dst, dev):
        return pltpu.make_async_remote_copy(src, dst, send_sem.at[SID[key]], recv_sem.at[SID[key]], device_id=dev, device_id_type=MESH)

    def same_size(key):
        piece = rs.at[0, 0] if key[0] == 'R' else full.at[0, 0, pl.ds(0, KROWS[key]), :]
        return remote(key, piece, piece, dev_p)

    def arrived(key):
        same_size(key).wait_recv()

    def own_pieces(i, side):
        la = int(i >= ATTN0[1])
        if i >= W_ITEM:
            if i == W_ITEM + 2:
                return [(wd.at[la, pl.ds(3 * BLK, BLK), :], 0, D)]
            cols = [1024 * (4 * (i - W_ITEM) + n) + 3 * BLK for n in range(4)]
        elif i in H_ITEMS:
            j = i - ATTN0[la] - 4
            cols = [m256(4096 * (n // 2) + 2048 * side + 1024 * (n % 2) + BLK * j) for n in range(4)]
        else:
            return [((wq, wk, wv, wo)[i - ATTN0[la]].at[la], 0, D)]
        out = []
        for n, c in enumerate(cols):
            out.append((wg.at[la, :, pl.ds(c, BLK)], n * TILE, BLK))
            out.append((wu.at[la, :, pl.ds(c, BLK)], n * TILE + BLK, BLK))
        return out

    def send_own(key, i, side, off, rows, dev):
        part = pl.ds(off, rows)
        for src, c0, nc in own_pieces(i, side):
            remote(key, src.at[part, :], full.at[i, me, part, pl.ds(c0, nc)], dev).start()

    def push(key, i, blk, off, dev):
        piece = full.at[i, blk, pl.ds(off, KROWS[key]), :]
        remote(key, piece, piece, dev).start()

    def push_n(key, i, off, dev):
        piece = full_n.at[H_ITEMS.index(i), n_y, pl.ds(off, KROWS[key]), :]
        remote(key, piece, piece, dev).start()

    def transfer(op):
        kind = op[0]
        if kind == 'wait':
            arrived(op[1])
        elif kind == 'drain':
            same_size(op[1]).wait_send()
        elif kind == 'ag':
            la, s = op[1:]
            remote(('H', la, s), h2.at[la, s, pl.ds(0, SEQ), :], h2.at[la, s, pl.ds(SEQ, SEQ), :], dev_x).start()
        elif kind == 'rs':
            la, s = op[1:]
            remote(('R', la, s), acc.at[s, pl.ds(SEQ, SEQ), :], rs.at[la, s], dev_x).start()
        else:
            i = op[1]
            px, py, dx, dy, pn = FLOW[ITEMS[i]]
            off_d = m16((BLK - dx - dy) * zz)
            if kind == 'ox':
                send_own(('X', i), i, 1 - xx, m16((BLK - px) * zz), px, dev_x)
            elif kind == 'oy':
                send_own(('Y', i), i, xx, m16((BLK - py) * zz), py, dev_y)
                send_own(('P0', i), i, xx, 0, BLK, dev_p)
            elif kind == 'fx':
                arrived(('X', i))
                if px < BLK:
                    push(('ZX', i), i, f_x, m16(px * zz), dev_z)
                else:
                    push(('P1', i), i, f_x, 0, dev_p)
                push(('DY', i), i, f_x, m16(off_d + dx), dev_y)
            elif kind == 'fy':
                arrived(('Y', i))
                push(('ZY', i), i, f_y, m16(py * zz), dev_z)
                if dx:
                    push(('DX', i), i, f_y, off_d, dev_x)
            elif kind == 'fd':
                if dx:
                    arrived(('DX', i))
                arrived(('DY', i))
                push(('ZD', i), i, f_d, m16((dx + dy) * zz), dev_z)
            elif kind == 'px':
                arrived(('ZX', i))
                push(('P1', i), i, f_x, 0, dev_p)
            elif kind == 'py':
                arrived(('ZY', i))
                push(('P2', i), i, f_y, 0, dev_p)
            elif kind == 'pd':
                arrived(('ZD', i))
                push(('P3', i), i, f_d, 0, dev_p)
            else:
                hn = H_ITEMS.index(i)
                la = int(i >= ATTN0[1])
                r0 = BLK * (i - ATTN0[la] - 4)
                if kind == 'on':
                    off = m16((BLK - pn) * zz)
                    remote(('N', i), wd.at[la, pl.ds(m16(r0 + off), pn), :], full_n.at[hn, n_me, pl.ds(off, pn), :], dev_y).start()
                    remote(('Q0', i), wd.at[la, pl.ds(r0, BLK), :], full_n.at[hn, n_me], dev_p).start()
                elif kind == 'fn':
                    arrived(('N', i))
                    push_n(('ZN', i), i, m16(pn * zz), dev_z)
                elif kind == 'pn':
                    arrived(('ZN', i))
                    push_n(('Q1', i), i, 0, dev_p)

    order, lists = plan()
    n_slot = len(order)

    def load(parts, slot):
        for src, dst in parts:
            pltpu.make_async_copy(src, dst, wt_sem.at[slot]).start()

    def others(i, n):
        slot = n % 2
        cols = pl.ds(n * TILE, TILE)
        load([(full.at[i, (me + k) % N_BLK, :, cols], wt.at[slot, (me + k) % N_BLK]) for k in range(1, N_BLK)], slot)

    def wait_tile(n, blocks=N_BLK):
        slot = n % 2
        part = wt.at[slot, pl.ds(0, blocks)]
        pltpu.make_async_copy(full.at[0, pl.ds(0, blocks), :, pl.ds(0, TILE)], part, wt_sem.at[slot]).wait()

    def load_mm(i, la, role, n):
        slot = n % 2
        cols = pl.ds(n * TILE, TILE)
        for k, w in enumerate((wq, wk, wv, wo)):
            pl.when(role == k)(functools.partial(load, [(w.at[la, :, cols], wt.at[slot, me])], slot))
        pl.when(role == 4)(functools.partial(load, [(wd.at[1, pl.ds(3 * BLK, BLK), cols], wt.at[slot, me])], slot))
        others(i, n)

    def load_gu(i, la, col, n):
        slot = n % 2
        c = pl.ds(m256(col(n)), BLK)
        load([(wg.at[la, :, c], wt.at[slot, me, :, pl.ds(0, BLK)]), (wu.at[la, :, c], wt.at[slot, me, :, pl.ds(BLK, BLK)])], slot)
        others(i, n)

    def load_dn(hn, la, j, n):
        slot = n % 2
        cols = pl.ds(n * TILE, TILE)
        parts = [(wd.at[la, pl.ds(m256(j * BLK), BLK), cols], wt.at[slot, n_me])]
        parts += [(full_n.at[hn, (n_me + k) % 4, :, cols], wt.at[slot, (n_me + k) % 4]) for k in range(1, 4)]
        load(parts, slot)

    def gain_row(la, k):
        return jnp.concatenate([gains[f, pl.ds(la * 4 + k, 1), :] for f in range(N_BLK)], axis=1)

    def scaled(v, gain):
        a = v.astype(jnp.bfloat16).astype(jnp.float32)
        ms = jnp.mean(a * a, axis=-1, keepdims=True)
        return a * lax.rsqrt(ms + EPS) * gain

    def rows(body):
        def step(r, carry):
            body(pl.multiple_of(r * RB, RB))
            return carry

        lax.fori_loop(0, SEQ // RB, step, 0)

    def act_rows(s, r0):
        return pl.ds(pl.multiple_of(s * SEQ + r0, RB), RB)

    def norm_rope(la, k, dst, s):
        gain = gain_row(la, k)

        def body(r0):
            v = scaled(acc[s, pl.ds(r0, RB), :], gain)
            c = cos_ref[pl.ds(r0, RB), :]
            sn = sin_ref[pl.ds(r0, RB), :]
            for h in range(D // HEAD_DIM):
                part = v[:, h * HEAD_DIM:(h + 1) * HEAD_DIM]
                turned = pltpu.roll(part, HEAD_DIM // 2, 1)
                act[dst, act_rows(s, r0), h * HEAD_DIM:(h + 1) * HEAD_DIM] = (part * c + turned * sn).astype(jnp.bfloat16)

        rows(body)

    def attention(q8, s):
        row = lax.broadcasted_iota(jnp.int32, (SEQ, SEQ), 0)
        col = lax.broadcasted_iota(jnp.int32, (SEQ, SEQ), 1)
        causal = row >= col
        sq = pl.ds(pl.multiple_of(s * SEQ, SEQ), SEQ)

        def step(h, carry):
            for u in range(2):
                lanes = pl.ds(pl.multiple_of((q8 * 8 + h * 2 + u) * HEAD_DIM, HEAD_DIM), HEAD_DIM)
                q, k, v = act[1, sq, lanes], act[2, sq, lanes], act[3, sq, lanes]
                sc = lax.dot_general(q, k, (((1,), (1,)), ((), ())), preferred_element_type=jnp.float32) * (HEAD_DIM ** -0.5)
                sc = jnp.where(causal, sc, -jnp.inf)
                e = jnp.exp(sc - jnp.max(sc, axis=-1, keepdims=True))
                p = (e / jnp.sum(e, axis=-1, keepdims=True)).astype(jnp.bfloat16)
                act[1, sq, lanes] = jnp.dot(p, v, preferred_element_type=jnp.float32).astype(jnp.bfloat16)
            return carry

        lax.fori_loop(0, 4, step, 0)

    def mm(i, la, role, hf):
        s0 = jnp.where(hf == 2, 0, hf)
        s1 = jnp.where(hf == 2, 2, hf + 1)
        lhs = jnp.where(role < 3, 0, jnp.where(role == 3, 1, 4))
        load_mm(i, la, role, 0)
        for n in range(N_TILE):
            if n + 1 < N_TILE:
                load_mm(i, la, role, n + 1)
            wait_tile(n)
            cols = slice(n * TILE, (n + 1) * TILE)

            def one(s, carry):
                left = act[lhs, pl.ds(pl.multiple_of(s * SEQ, SEQ), SEQ), :]
                prod = jnp.dot(left, wt[n % 2].reshape(D, TILE), preferred_element_type=jnp.float32)
                acc[s, :SEQ, cols] = jnp.where(role == 4, acc[s, :SEQ, cols], 0.0) + prod
                return carry

            lax.fori_loop(s0, s1, one, 0)

        def epilogue(s, carry):
            @pl.when(role == 0)
            def _():
                norm_rope(la, 0, 1, s)

            @pl.when(role == 1)
            def _():
                norm_rope(la, 1, 2, s)

            @pl.when(role == 2)
            def _():
                def body(r0):
                    act[3, act_rows(s, r0), :] = acc[s, pl.ds(r0, RB), :].astype(jnp.bfloat16)

                rows(body)

            @pl.when(role == 3)
            def _():
                gain = gain_row(la, 2)

                def body(r0):
                    h = act[0, act_rows(s, r0), :].astype(jnp.float32) + scaled(acc[s, pl.ds(r0, RB), :], gain)
                    h2[la, s, pl.ds(r0, RB), :] = h.astype(jnp.bfloat16)

                rows(body)

            return carry

        lax.fori_loop(s0, s1, epilogue, 0)

    def swiglu(prod):
        gate = prod[:, :BLK].astype(jnp.bfloat16).astype(jnp.float32)
        up = prod[:, BLK:].astype(jnp.bfloat16).astype(jnp.float32)
        return (jax.nn.silu(gate) * up).astype(jnp.bfloat16)

    def shared_mlp(i, hn, la, j, s):
        def col(n):
            return 4096 * (n // 2) + 2048 * xx + 1024 * (n % 2) + BLK * j

        load_gu(i, la, col, 0)
        for n in range(N_TILE):
            if n + 1 < N_TILE:
                load_gu(i, la, col, n + 1)
            else:
                load_dn(hn, la, j, 0)
            wait_tile(n)
            prod = jnp.dot(h2[la, s], wt[n % 2].reshape(D, TILE), preferred_element_type=jnp.float32)
            mj[:, n * BLK:(n + 1) * BLK] = swiglu(prod)
        for n in range(N_TILE):
            if n + 1 < N_TILE:
                load_dn(hn, la, j, n + 1)
            wait_tile(n, 4)
            cols = slice(n * TILE, (n + 1) * TILE)
            prod = jnp.dot(mj[...], wt[n % 2, :4].reshape(4 * BLK, TILE), preferred_element_type=jnp.float32)
            acc[s, :, cols] = jnp.where(j > 0, acc[s, :, cols], 0.0) + prod

    def plain_gu(i, e):
        def col(n):
            return 1024 * (4 * e + n) + 3 * BLK

        load_gu(i, 1, col, 0)
        for n in range(N_TILE):
            if n + 1 < N_TILE:
                load_gu(i, 1, col, n + 1)
            wait_tile(n)

            def one(s, carry):
                prod = jnp.dot(h2[1, s, :SEQ], wt[n % 2].reshape(D, TILE), preferred_element_type=jnp.float32)
                act[4, pl.ds(pl.multiple_of(s * SEQ, SEQ), SEQ), pl.ds(m256(e * 1024 + n * BLK), BLK)] = swiglu(prod)
                return carry

            lax.fori_loop(0, 2, one, 0)

    def finish(la, s):
        gain = gain_row(la, 3)

        def body(r0):
            y = scaled(acc[s, pl.ds(r0, RB), :] + rs[la, s, pl.ds(r0, RB), :], gain)
            act[0, act_rows(s, r0), :] = (h2[la, s, pl.ds(r0, RB), :].astype(jnp.float32) + y).astype(jnp.bfloat16)

        rows(body)

    def pick(p, values):
        out = jnp.int32(0)
        for k, v in enumerate(values):
            if v:
                out = jnp.where(p == k, v, out)
        return out

    gain_copies = []
    for k in range(1, N_BLK):
        cp = pltpu.make_async_remote_copy(gain_ref, gains.at[me], gs_sem.at[k], gr_sem.at[k], device_id=(zz, (me + k) % N_BLK), device_id_type=MESH)
        gain_copies.append(cp)

    types = ['mm', 'at', 'h', 'wgu', 'wd', 'fin']

    def step(p, carry):
        for k in range(n_slot):
            if not lists[k]:
                continue

            @pl.when(p == k)
            def _(k=k):
                if k == 0:
                    for cp in gain_copies:
                        cp.start()
                for op in lists[k]:
                    transfer(op)
                if k == 0:
                    x_copy.wait()
                    for cp in gain_copies:
                        cp.wait()
                    gains[pl.ds(me, 1)] = gain_ref[...][None]

        ty = pick(p, [types.index(o[0]) for o in order])
        item = pick(p, [o[1] for o in order])
        la = pick(p, [o[2] for o in order])
        ex = pick(p, [o[3] for o in order])
        hf = pick(p, [o[4] for o in order])
        hn = pick(p, [H_ITEMS.index(o[1]) if o[0] == 'h' else 0 for o in order])
        pl.when((ty == 0) | (ty == 4))(lambda: mm(item, la, ex, hf))
        pl.when(ty == 1)(lambda: attention(ex, hf))
        pl.when(ty == 2)(lambda: shared_mlp(item, hn, la, ex, hf))
        pl.when(ty == 3)(lambda: plain_gu(item, ex))
        pl.when(ty == 5)(lambda: finish(la, hf))
        return carry

    lax.fori_loop(0, n_slot, step, 0)

    out_copy = pltpu.make_async_copy(act.at[0], out_hbm, io_sem)
    out_copy.start()
    drained = [op[1] for ops in lists for op in ops if op[0] == 'drain']
    for key, _ in KEYS:
        if key not in drained:
            same_size(key).wait_send()
    out_copy.wait()


def solution(mesh):
    cos_np, sin_np = rope_tables()
    hbm = pl.BlockSpec(memory_space=pl.ANY)
    vmem = pl.BlockSpec(memory_space=pltpu.VMEM)
    n_copy = len(KEYS)

    def local_fn(tokens, weights, gain_vecs):
        gains = jnp.stack(gain_vecs, axis=1).reshape(8, BLK).astype(jnp.float32)
        flat = tokens.reshape(ROWS, D)
        out = pl.pallas_call(
            kernel,
            out_shape=(
                jax.ShapeDtypeStruct((ROWS, D), jnp.bfloat16),
                jax.ShapeDtypeStruct((len(ITEMS), N_BLK, BLK, D), jnp.bfloat16),
                jax.ShapeDtypeStruct((len(H_ITEMS), 4, BLK, D), jnp.bfloat16),
            ),
            in_specs=[hbm, vmem, vmem, vmem] + [hbm] * 7,
            out_specs=(hbm, hbm, hbm),
            scratch_shapes=[
                pltpu.VMEM((5, ROWS, D), jnp.bfloat16),
                pltpu.VMEM((2, 2, 2 * SEQ, D), jnp.bfloat16),
                pltpu.VMEM((2 * SEQ, 4 * BLK), jnp.bfloat16),
                pltpu.VMEM((2, 2 * SEQ, D), jnp.float32),
                pltpu.VMEM((2, 2, SEQ, D), jnp.float32),
                pltpu.VMEM((2, N_BLK, BLK, TILE), jnp.bfloat16),
                pltpu.VMEM((N_BLK, 8, BLK), jnp.float32),
                pltpu.SemaphoreType.DMA((n_copy,)),
                pltpu.SemaphoreType.DMA((n_copy,)),
                pltpu.SemaphoreType.DMA((2,)),
                pltpu.SemaphoreType.DMA((N_BLK,)),
                pltpu.SemaphoreType.DMA((N_BLK,)),
                pltpu.SemaphoreType.DMA,
            ],
            compiler_params=pltpu.CompilerParams(collective_id=0, has_side_effects=True, vmem_limit_bytes=60 * 1024 * 1024),
        )(flat, jnp.asarray(cos_np), jnp.asarray(sin_np), gains, *weights)
        return out[0].reshape(tokens.shape)

    mapped = jax.shard_map(local_fn, mesh=mesh, in_specs=(P(('dp', 'fsdp')), P(None, 'fsdp'), P(None, 'fsdp')), out_specs=P(('dp', 'fsdp')), check_vma=False)

    def run(tokens, w_query, w_key, w_value, w_out, w_gate, w_up, w_down, g_query, g_key, g_attn, g_mlp):
        return mapped(tokens, (w_query, w_key, w_value, w_out, w_gate, w_up, w_down), (g_query, g_key, g_attn, g_mlp))

    return run
```

```python
import functools

import jax
import jax.numpy as jnp
import numpy as np
from jax import lax
from jax.experimental import pallas as pl
from jax.experimental.pallas import tpu as pltpu
from jax.sharding import PartitionSpec as P

HEAD_DIM = 128
EPS = 1e-6
THETA = 500000.0
SEQ = 256
D = 2048
ROWS = 512
N_BLK = 8
BLK = 256
TILE = 512
N_TILE = D // TILE
RB = 32
MESH = pl.DeviceIdType.MESH

UNIT = 22.5 / 256
LAT = 2.5
PAIR = 4.0
AXES = {'A': 'xy', 'B': 'xy', 'C': 'xy', 'H': 'xy', 'G': 'xy'}
FLOW = {'A': (208, 144, 96, 48, 0), 'B': (128, 160, 0, 128, 0), 'C': (144, 192, 0, 144, 0), 'H': (208, 176, 0, 144, 128), 'G': (160, 144, 0, 128, 192)}
ITEMS = ['A'] * 4 + ['H'] * 4 + ['B'] * 4 + ['G'] * 3 + ['C'] * 3
BACKLOG = 18.0
N_H = (4, 3)
COST = {'mm': 6.6, 'at': 4.5, 'h': 10.5, 'wgu': 7.5, 'wd': 11.0, 'fin': 1.5}
BOTH = {'mm': 11.0, 'h': 11.6, 'wgu': 7.5, 'wd': 11.0}


def slots(nh=N_H):
    out = []
    for k in range(3):
        out.append(('mm', k, 0, k, 2))
    attn = (0, 4 + nh[0])
    for s in range(2):
        for q in range(2):
            out.append(('at', 0, 0, q, s))
        out.append(('mm', 3, 0, 3, s))
    for j in range(nh[0]):
        for s in range(2):
            out.append(('h', 4 + j, 0, j, s))
    for s in range(2):
        out.append(('fin', 0, 0, 0, s))
    a1 = attn[1]
    h0 = a1 + 4
    for s in range(2):
        for k in range(3):
            out.append(('mm', a1 + k, 1, k, s))
        for q in range(2):
            out.append(('at', 0, 1, q, s))
        out.append(('mm', a1 + 3, 1, 3, s))
    for s in range(2):
        for j in range(nh[1]):
            out.append(('h', h0 + j, 1, j, s))
    w0 = h0 + nh[1]
    if nh[1] < 4:
        out.append(('wgu', w0, 1, 0, 2))
        out.append(('wgu', w0 + 1, 1, 1, 2))
        out.append(('wd', w0 + 2, 1, 4, 2))
    for s in range(2):
        out.append(('fin', 0, 1, 0, s))
    return out


def schedule(thr=20.0, nh=N_H):
    sl = slots(nh)
    t = 0.0
    free = dict(x=0.0, y=0.0, z=0.0, p=0.0)
    arr = {}
    prog = []
    busy = dict(x=0.0, y=0.0, z=0.0, p=0.0)

    def send(link, dur, key):
        s = max(free[link], t)
        free[link] = s + dur
        busy[link] += dur
        arr[key] = free[link] + LAT

    todo_send = {}
    for i, f in enumerate(ITEMS):
        px, py, dx, dy, pn = FLOW[f]
        a, b = AXES[f]

        def add(k, link, dur, *deps):
            todo_send[(k, i)] = (i, link, dur, [(d, i) for d in deps])

        add('X', a, px * UNIT)
        add('Y', b, py * UNIT)
        add('P0', 'p', PAIR)
        add('DY', b, dy * UNIT, 'X')
        if dx:
            add('DX', a, dx * UNIT, 'Y')
        if px < 256:
            add('ZX', 'z', (256 - px) * UNIT, 'X')
            add('P1', 'p', PAIR, 'X', 'ZX')
        else:
            add('P1', 'p', PAIR, 'X')
        add('ZY', 'z', (256 - py) * UNIT, 'Y')
        add('P2', 'p', PAIR, 'Y', 'ZY')
        diag = ('DX', 'DY') if dx else ('DY',)
        add('ZD', 'z', (256 - dx - dy) * UNIT, *diag)
        add('P3', 'p', PAIR, *(diag + ('ZD',)))
        if pn:
            add('N', b, pn * UNIT)
            add('Q0', 'p', PAIR)
            add('ZN', 'z', (256 - pn) * UNIT, 'N')
            add('Q1', 'p', PAIR, 'N', 'ZN')
    limit = dict(x=thr, y=thr, z=thr, p=2 * PAIR)

    def needs(s):
        ty, it, la, ex, hf = s
        n = []
        if ty in ('mm', 'h', 'wgu', 'wd'):
            n += [('P%d' % k, it) for k in range(4)]
        if ty == 'h':
            n += [('Q%d' % k, it) for k in range(2)]
            n.append(('H', la, hf))
        if ty == 'fin':
            n.append(('R', la, hf))
        return n

    def after(s):
        ty, it, la, ex, hf = s
        halves = [hf] if hf < 2 else [0, 1]
        if ty == 'mm' and ex < 3:
            return [('fin', la - 1, 0, hf)] if la else []
        if ty == 'at':
            return [('mm', la, k, hf if la else 2) for k in range(3)]
        if ty == 'mm':
            return [('at', la, q, hf) for q in range(2)]
        if ty == 'h':
            return [('mm', la, 3, q) for q in halves] + ([('h', la, ex - 1, hf)] if ex else [])
        if ty == 'wgu':
            return [('mm', la, 3, 0), ('mm', la, 3, 1)]
        if ty == 'wd':
            return [('wgu', la, 0, 2), ('wgu', la, 1, 2)] + [('h', la, nh[1] - 1, q) for q in range(2)]
        return [('h', la, nh[la] - 1, hf)] + ([('wd', la, 4, 2)] if la and nh[1] < 4 else [])

    done = set()
    todo = list(range(len(sl)))
    while todo:
        again = True
        while again:
            again = False
            ready = {}
            for key, (pri, link, dur, deps) in todo_send.items():
                if free[link] - t < limit[link] and all(arr.get(x, 1e9) <= t for x in deps):
                    if link not in ready or (pri, len(deps) == 0) < ready[link][0]:
                        ready[link] = ((pri, len(deps) == 0), key)
            for link, (_, key) in ready.items():
                send(link, todo_send[key][2], key)
                prog.append(('send', key, todo_send.pop(key)[3]))
                again = True
        pick = None
        ev = [arr[x] for e in todo_send.values() for x in e[3] if x in arr]
        ev += [free[e[1]] - limit[e[1]] + 0.01 for e in todo_send.values()]
        for k in todo:
            s = sl[k]
            if not all(x in done for x in after(s)):
                continue
            ns = needs(s)
            if all(arr.get(x, 1e9) <= t for x in ns):
                pick = k
                break
            ev += [arr[x] for x in ns if x in arr]
        if pick is not None:
            s = sl[pick]
            todo.remove(pick)
            prog.append(('slot', pick))
            t += BOTH[s[0]] if s[4] == 2 else COST[s[0]]
            done.add((s[0], s[2], s[3], s[4]))
            halves = [s[4]] if s[4] < 2 else [0, 1]
            for q in halves:
                key = None
                if s[0] == 'mm' and s[3] == 3:
                    key, units = ('H', s[2], q), 1
                if s[0] == 'h' and s[3] == nh[s[2]] - 1:
                    key, units = ('R', s[2], q), 2
                if key:
                    todo_send[key] = (-1, AXES['HG'[s[2]]][0], units * 22.5, [])
            continue
        t = min(e for e in ev if e > t)
    assert not todo_send
    return sl, prog, t


def plan():
    sl, prog, _ = schedule(BACKLOG, N_H)
    order, lists, cur, seen = [], [], [], set()

    def await_all(keys):
        for key in keys:
            if key not in seen:
                seen.add(key)
                cur.append(('wait', key))

    for op in prog:
        if op[0] == 'send':
            await_all(op[2])
            cur.append(('send', op[1]))
            continue
        s = sl[op[1]]
        ty, it, la, ex, hf = s
        if ty in ('mm', 'h', 'wgu', 'wd'):
            await_all([('P%d' % k, it) for k in range(4)])
        if ty == 'h':
            await_all([('Q%d' % k, it) for k in range(2)])
            await_all([('H', la, hf)])
            if la == 1 and ex == 0:
                cur.append(('drain', ('R', 0, hf)))
        if ty == 'fin':
            await_all([('R', la, hf)])
        order.append(s)
        lists.append(cur)
        cur = []
    assert not cur and all(k in seen for k, _ in KEYS)
    return order, lists


def copy_keys():
    keys = []
    for i, f in enumerate(ITEMS):
        px, py, dx, dy, pn = FLOW[f]
        rows = {'X': px, 'Y': py, 'P0': BLK, 'DX': dx, 'DY': dy, 'ZX': BLK - px, 'ZY': BLK - py, 'ZD': BLK - dx - dy, 'P1': BLK, 'P2': BLK, 'P3': BLK}
        if pn:
            rows.update({'N': pn, 'ZN': BLK - pn, 'Q0': BLK, 'Q1': BLK})
        keys += [((k, i), r) for k, r in rows.items() if r]
    for la in range(2):
        for s in range(2):
            keys += [(('H', la, s), BLK), (('R', la, s), 0)]
    return keys


KEYS = copy_keys()
SID = {k: n for n, (k, _) in enumerate(KEYS)}
KROWS = dict(KEYS)
H_ITEMS = [i for i, f in enumerate(ITEMS) if FLOW[f][4]]
ATTN0 = (0, 4 + N_H[0])
W_ITEM = 8 + N_H[0] + N_H[1]


def rope_tables():
    pos = np.arange(SEQ, dtype=np.float64)
    inv = THETA ** (-2.0 * np.arange(HEAD_DIM // 2, dtype=np.float64) / HEAD_DIM)
    ang = pos[:, None] * inv[None, :]
    cos, sin = np.cos(ang), np.sin(ang)
    return (np.concatenate([cos, cos], 1).astype(np.float32), np.concatenate([-sin, sin], 1).astype(np.float32))


def kernel(x_hbm, cos_ref, sin_ref, gq, gk, ga, gm, wq, wk, wv, wo, wg, wu, wd, out_hbm, full, full_n, act, h2, mj, acc, rs, wt, gains, gain_in, gain_ref, send_sem, recv_sem, wt_sem, gs_sem, gr_sem, io_sem, gi_sem):
    zz = lax.axis_index('dp')
    me = lax.axis_index('fsdp')
    cc = me % 2
    xx = (me // 2) % 2
    yy = me // 4

    def at(y, x, c):
        return y * 4 + x * 2 + c

    f_p = at(yy, xx, 1 - cc)
    f_x = at(yy, 1 - xx, cc)
    f_y = at(1 - yy, xx, cc)
    f_d = at(1 - yy, 1 - xx, cc)
    n_me, n_y = yy * 2 + cc, (1 - yy) * 2 + cc
    dev_p, dev_x, dev_y, dev_z = (zz, f_p), (zz, f_x), (zz, f_y), (1 - zz, me)

    x_copy = pltpu.make_async_copy(x_hbm, act.at[0], io_sem)
    x_copy.start()

    gain_loads = [pltpu.make_async_copy(g, gain_in.at[k], gi_sem.at[k]) for k, g in enumerate((gq, gk, ga, gm))]
    for cp in gain_loads:
        cp.start()
    for k, cp in enumerate(gain_loads):
        cp.wait()
        for la in range(2):
            gain_ref[la * 4 + k:la * 4 + k + 1, :] = gain_in[k, la:la + 1, :].astype(jnp.float32)

    barrier = pltpu.get_barrier_semaphore()
    for k in range(1, N_BLK):
        pl.semaphore_signal(barrier, inc=1, device_id=(zz, (me + k) % N_BLK), device_id_type=MESH)
    pl.semaphore_signal(barrier, inc=1, device_id=dev_z, device_id_type=MESH)
    pl.semaphore_wait(barrier, N_BLK)

    def m16(v):
        return pl.multiple_of(v, 16)

    def m256(v):
        return pl.multiple_of(v, 256)

    def remote(key, src, dst, dev):
        return pltpu.make_async_remote_copy(src, dst, send_sem.at[SID[key]], recv_sem.at[SID[key]], device_id=dev, device_id_type=MESH)

    def same_size(key):
        piece = rs.at[0, 0] if key[0] == 'R' else full.at[0, 0, pl.ds(0, KROWS[key]), :]
        return remote(key, piece, piece, dev_p)

    def arrived(key):
        same_size(key).wait_recv()

    def own_pieces(i, side):
        la = int(i >= ATTN0[1])
        if i >= W_ITEM:
            if i == W_ITEM + 2:
                return [(wd.at[la, pl.ds(3 * BLK, BLK), :], 0, D)]
            cols = [1024 * (4 * (i - W_ITEM) + n) + 3 * BLK for n in range(4)]
        elif i in H_ITEMS:
            j = i - ATTN0[la] - 4
            cols = [m256(4096 * (n // 2) + 2048 * side + 1024 * (n % 2) + BLK * j) for n in range(4)]
        else:
            return [((wq, wk, wv, wo)[i - ATTN0[la]].at[la], 0, D)]
        out = []
        for n, c in enumerate(cols):
            out.append((wg.at[la, :, pl.ds(c, BLK)], n * TILE, BLK))
            out.append((wu.at[la, :, pl.ds(c, BLK)], n * TILE + BLK, BLK))
        return out

    def send_own(key, side, off, dev):
        i = key[1]
        part = pl.ds(off, KROWS[key])
        for src, c0, nc in own_pieces(i, side):
            remote(key, src.at[part, :], full.at[i, me, part, pl.ds(c0, nc)], dev).start()

    def push(key, blk, off, dev):
        piece = full.at[key[1], blk, pl.ds(off, KROWS[key]), :]
        remote(key, piece, piece, dev).start()

    def push_n(key, off, dev):
        piece = full_n.at[H_ITEMS.index(key[1]), n_y, pl.ds(off, KROWS[key]), :]
        remote(key, piece, piece, dev).start()

    def own_n(key, off, dev):
        i = key[1]
        la = int(i >= ATTN0[1])
        r0 = BLK * (i - ATTN0[la] - 4)
        rr = KROWS[key]
        remote(key, wd.at[la, pl.ds(m16(r0 + off), rr), :], full_n.at[H_ITEMS.index(i), n_me, pl.ds(off, rr), :], dev).start()

    def transfer(op):
        key = op[1]
        if op[0] == 'wait':
            return arrived(key)
        if op[0] == 'drain':
            return same_size(key).wait_send()
        kind = key[0]
        if kind == 'H':
            la, s = key[1:]
            return remote(key, h2.at[la, s, pl.ds(0, SEQ), :], h2.at[la, s, pl.ds(SEQ, SEQ), :], dev_x).start()
        if kind == 'R':
            la, s = key[1:]
            return remote(key, acc.at[s, pl.ds(SEQ, SEQ), :], rs.at[la, s], dev_x).start()
        px, py, dx, dy, pn = FLOW[ITEMS[key[1]]]
        off_d = m16((BLK - dx - dy) * zz)
        steps = {
            'X': lambda: send_own(key, 1 - xx, m16((BLK - px) * zz), dev_x),
            'Y': lambda: send_own(key, xx, m16((BLK - py) * zz), dev_y),
            'P0': lambda: send_own(key, xx, 0, dev_p),
            'ZX': lambda: push(key, f_x, m16(px * zz), dev_z),
            'ZY': lambda: push(key, f_y, m16(py * zz), dev_z),
            'ZD': lambda: push(key, f_d, m16((dx + dy) * zz), dev_z),
            'DX': lambda: push(key, f_y, off_d, dev_x),
            'DY': lambda: push(key, f_x, m16(off_d + dx), dev_y),
            'P1': lambda: push(key, f_x, 0, dev_p),
            'P2': lambda: push(key, f_y, 0, dev_p),
            'P3': lambda: push(key, f_d, 0, dev_p),
            'N': lambda: own_n(key, m16((BLK - pn) * zz), dev_y),
            'Q0': lambda: own_n(key, 0, dev_p),
            'ZN': lambda: push_n(key, m16(pn * zz), dev_z),
            'Q1': lambda: push_n(key, 0, dev_p),
        }
        steps[kind]()

    order, lists = plan()
    n_slot = len(order)

    def load(parts, slot):
        for src, dst in parts:
            pltpu.make_async_copy(src, dst, wt_sem.at[slot]).start()

    def others(i, n):
        slot = n % 2
        cols = pl.ds(n * TILE, TILE)
        load([(full.at[i, (me + k) % N_BLK, :, cols], wt.at[slot, (me + k) % N_BLK]) for k in range(1, N_BLK)], slot)

    def wait_tile(n, blocks=N_BLK):
        slot = n % 2
        part = wt.at[slot, pl.ds(0, blocks)]
        pltpu.make_async_copy(full.at[0, pl.ds(0, blocks), :, pl.ds(0, TILE)], part, wt_sem.at[slot]).wait()

    def load_mm(i, la, role, n):
        slot = n % 2
        cols = pl.ds(n * TILE, TILE)
        for k, w in enumerate((wq, wk, wv, wo)):
            pl.when(role == k)(functools.partial(load, [(w.at[la, :, cols], wt.at[slot, me])], slot))
        pl.when(role == 4)(functools.partial(load, [(wd.at[1, pl.ds(3 * BLK, BLK), cols], wt.at[slot, me])], slot))
        others(i, n)

    def load_gu(i, la, col, n):
        slot = n % 2
        c = pl.ds(m256(col(n)), BLK)
        load([(wg.at[la, :, c], wt.at[slot, me, :, pl.ds(0, BLK)]), (wu.at[la, :, c], wt.at[slot, me, :, pl.ds(BLK, BLK)])], slot)
        others(i, n)

    def load_dn(hn, la, j, n):
        slot = n % 2
        cols = pl.ds(n * TILE, TILE)
        parts = [(wd.at[la, pl.ds(m256(j * BLK), BLK), cols], wt.at[slot, n_me])]
        parts += [(full_n.at[hn, (n_me + k) % 4, :, cols], wt.at[slot, (n_me + k) % 4]) for k in range(1, 4)]
        load(parts, slot)

    def gain_row(la, k):
        return jnp.concatenate([gains[f, pl.ds(la * 4 + k, 1), :] for f in range(N_BLK)], axis=1)

    def scaled(v, gain):
        a = v.astype(jnp.bfloat16).astype(jnp.float32)
        ms = jnp.mean(a * a, axis=-1, keepdims=True)
        return a * lax.rsqrt(ms + EPS) * gain

    def rows(body):
        def step(r, carry):
            body(pl.multiple_of(r * RB, RB))
            return carry

        lax.fori_loop(0, SEQ // RB, step, 0)

    def act_rows(s, r0):
        return pl.ds(pl.multiple_of(s * SEQ + r0, RB), RB)

    def norm_rope(la, k, dst, s):
        gain = gain_row(la, k)

        def body(r0):
            v = scaled(acc[s, pl.ds(r0, RB), :], gain)
            c = cos_ref[pl.ds(r0, RB), :]
            sn = sin_ref[pl.ds(r0, RB), :]
            for h in range(D // HEAD_DIM):
                part = v[:, h * HEAD_DIM:(h + 1) * HEAD_DIM]
                turned = pltpu.roll(part, HEAD_DIM // 2, 1)
                act[dst, act_rows(s, r0), h * HEAD_DIM:(h + 1) * HEAD_DIM] = (part * c + turned * sn).astype(jnp.bfloat16)

        rows(body)

    def attention(q8, s):
        row = lax.broadcasted_iota(jnp.int32, (SEQ, SEQ), 0)
        col = lax.broadcasted_iota(jnp.int32, (SEQ, SEQ), 1)
        causal = row >= col
        sq = pl.ds(pl.multiple_of(s * SEQ, SEQ), SEQ)

        def step(h, carry):
            for u in range(2):
                lanes = pl.ds(pl.multiple_of((q8 * 8 + h * 2 + u) * HEAD_DIM, HEAD_DIM), HEAD_DIM)
                q, k, v = act[1, sq, lanes], act[2, sq, lanes], act[3, sq, lanes]
                sc = lax.dot_general(q, k, (((1,), (1,)), ((), ())), preferred_element_type=jnp.float32) * (HEAD_DIM ** -0.5)
                sc = jnp.where(causal, sc, -jnp.inf)
                e = jnp.exp(sc - jnp.max(sc, axis=-1, keepdims=True))
                p = (e / jnp.sum(e, axis=-1, keepdims=True)).astype(jnp.bfloat16)
                act[1, sq, lanes] = jnp.dot(p, v, preferred_element_type=jnp.float32).astype(jnp.bfloat16)
            return carry

        lax.fori_loop(0, 4, step, 0)

    def mm(i, la, role, hf):
        s0 = jnp.where(hf == 2, 0, hf)
        s1 = jnp.where(hf == 2, 2, hf + 1)
        lhs = jnp.where(role < 3, 0, jnp.where(role == 3, 1, 4))
        load_mm(i, la, role, 0)
        for n in range(N_TILE):
            if n + 1 < N_TILE:
                load_mm(i, la, role, n + 1)
            wait_tile(n)
            cols = slice(n * TILE, (n + 1) * TILE)

            def one(s, carry):
                left = act[lhs, pl.ds(pl.multiple_of(s * SEQ, SEQ), SEQ), :]
                prod = jnp.dot(left, wt[n % 2].reshape(D, TILE), preferred_element_type=jnp.float32)
                acc[s, :SEQ, cols] = jnp.where(role == 4, acc[s, :SEQ, cols], 0.0) + prod
                return carry

            lax.fori_loop(s0, s1, one, 0)

        def epilogue(s, carry):
            @pl.when(role == 0)
            def _():
                norm_rope(la, 0, 1, s)

            @pl.when(role == 1)
            def _():
                norm_rope(la, 1, 2, s)

            @pl.when(role == 2)
            def _():
                def body(r0):
                    act[3, act_rows(s, r0), :] = acc[s, pl.ds(r0, RB), :].astype(jnp.bfloat16)

                rows(body)

            @pl.when(role == 3)
            def _():
                gain = gain_row(la, 2)

                def body(r0):
                    h = act[0, act_rows(s, r0), :].astype(jnp.float32) + scaled(acc[s, pl.ds(r0, RB), :], gain)
                    h2[la, s, pl.ds(r0, RB), :] = h.astype(jnp.bfloat16)

                rows(body)

            return carry

        lax.fori_loop(s0, s1, epilogue, 0)

    def swiglu(prod):
        gate = prod[:, :BLK].astype(jnp.bfloat16).astype(jnp.float32)
        up = prod[:, BLK:].astype(jnp.bfloat16).astype(jnp.float32)
        return (jax.nn.silu(gate) * up).astype(jnp.bfloat16)

    def halves(hf):
        return jnp.where(hf == 2, 0, hf), jnp.where(hf == 2, 2, hf + 1)

    def shared_mlp(i, hn, la, j, s):
        def col(n):
            return 4096 * (n // 2) + 2048 * xx + 1024 * (n % 2) + BLK * j

        load_gu(i, la, col, 0)
        for n in range(N_TILE):
            if n + 1 < N_TILE:
                load_gu(i, la, col, n + 1)
            else:
                load_dn(hn, la, j, 0)
            wait_tile(n)
            prod = jnp.dot(h2[la, s], wt[n % 2].reshape(D, TILE), preferred_element_type=jnp.float32)
            mj[:, n * BLK:(n + 1) * BLK] = swiglu(prod)
        for n in range(N_TILE):
            if n + 1 < N_TILE:
                load_dn(hn, la, j, n + 1)
            wait_tile(n, 4)
            cols = slice(n * TILE, (n + 1) * TILE)
            prod = jnp.dot(mj[...], wt[n % 2, :4].reshape(4 * BLK, TILE), preferred_element_type=jnp.float32)
            acc[s, :, cols] = jnp.where(j > 0, acc[s, :, cols], 0.0) + prod

    def plain_gu(i, e):
        def col(n):
            return 1024 * (4 * e + n) + 3 * BLK

        load_gu(i, 1, col, 0)
        for n in range(N_TILE):
            if n + 1 < N_TILE:
                load_gu(i, 1, col, n + 1)
            wait_tile(n)

            def one(s, carry):
                prod = jnp.dot(h2[1, s, :SEQ], wt[n % 2].reshape(D, TILE), preferred_element_type=jnp.float32)
                act[4, pl.ds(pl.multiple_of(s * SEQ, SEQ), SEQ), pl.ds(m256(e * 1024 + n * BLK), BLK)] = swiglu(prod)
                return carry

            lax.fori_loop(0, 2, one, 0)

    def finish(la, s):
        gain = gain_row(la, 3)

        def body(r0):
            y = scaled(acc[s, pl.ds(r0, RB), :] + rs[la, s, pl.ds(r0, RB), :], gain)
            act[0, act_rows(s, r0), :] = (h2[la, s, pl.ds(r0, RB), :].astype(jnp.float32) + y).astype(jnp.bfloat16)

        rows(body)

    def pick(p, values):
        out = jnp.int32(0)
        for k, v in enumerate(values):
            if v:
                out = jnp.where(p == k, v, out)
        return out

    gain_copies = []
    for k in range(1, N_BLK):
        cp = pltpu.make_async_remote_copy(gain_ref, gains.at[me], gs_sem.at[k], gr_sem.at[k], device_id=(zz, (me + k) % N_BLK), device_id_type=MESH)
        gain_copies.append(cp)

    types = ['mm', 'at', 'h', 'wgu', 'wd', 'fin']

    def step(p, carry):
        for k in range(n_slot):
            if not lists[k]:
                continue

            @pl.when(p == k)
            def _(k=k):
                if k == 0:
                    for cp in gain_copies:
                        cp.start()
                for op in lists[k]:
                    transfer(op)
                if k == 0:
                    x_copy.wait()
                    for cp in gain_copies:
                        cp.wait()
                    gains[pl.ds(me, 1)] = gain_ref[...][None]

        ty = pick(p, [types.index(o[0]) for o in order])
        item = pick(p, [o[1] for o in order])
        la = pick(p, [o[2] for o in order])
        ex = pick(p, [o[3] for o in order])
        hf = pick(p, [o[4] for o in order])
        hn = pick(p, [H_ITEMS.index(o[1]) if o[0] == 'h' else 0 for o in order])
        pl.when((ty == 0) | (ty == 4))(lambda: mm(item, la, ex, hf))
        pl.when(ty == 1)(lambda: attention(ex, hf))
        pl.when(ty == 2)(lambda: shared_mlp(item, hn, la, ex, hf))
        pl.when(ty == 3)(lambda: plain_gu(item, ex))
        pl.when(ty == 5)(lambda: finish(la, hf))
        return carry

    lax.fori_loop(0, n_slot, step, 0)

    out_copy = pltpu.make_async_copy(act.at[0], out_hbm, io_sem)
    out_copy.start()
    drained = [op[1] for ops in lists for op in ops if op[0] == 'drain']
    for key, _ in KEYS:
        if key not in drained:
            same_size(key).wait_send()
    out_copy.wait()


def solution(mesh):
    cos_np, sin_np = rope_tables()
    hbm = pl.BlockSpec(memory_space=pl.ANY)
    vmem = pl.BlockSpec(memory_space=pltpu.VMEM)
    n_copy = len(KEYS)

    def local_fn(tokens, weights, gain_vecs):
        flat = tokens.reshape(ROWS, D)
        out = pl.pallas_call(
            kernel,
            out_shape=(
                jax.ShapeDtypeStruct((ROWS, D), jnp.bfloat16),
                jax.ShapeDtypeStruct((len(ITEMS), N_BLK, BLK, D), jnp.bfloat16),
                jax.ShapeDtypeStruct((len(H_ITEMS), 4, BLK, D), jnp.bfloat16),
            ),
            in_specs=[hbm, vmem, vmem] + [hbm] * 11,
            out_specs=(hbm, hbm, hbm),
            scratch_shapes=[
                pltpu.VMEM((5, ROWS, D), jnp.bfloat16),
                pltpu.VMEM((2, 2, 2 * SEQ, D), jnp.bfloat16),
                pltpu.VMEM((2 * SEQ, 4 * BLK), jnp.bfloat16),
                pltpu.VMEM((2, 2 * SEQ, D), jnp.float32),
                pltpu.VMEM((2, 2, SEQ, D), jnp.float32),
                pltpu.VMEM((2, N_BLK, BLK, TILE), jnp.bfloat16),
                pltpu.VMEM((N_BLK, 8, BLK), jnp.float32),
                pltpu.VMEM((4, 2, BLK), jnp.bfloat16),
                pltpu.VMEM((8, BLK), jnp.float32),
                pltpu.SemaphoreType.DMA((n_copy,)),
                pltpu.SemaphoreType.DMA((n_copy,)),
                pltpu.SemaphoreType.DMA((2,)),
                pltpu.SemaphoreType.DMA((N_BLK,)),
                pltpu.SemaphoreType.DMA((N_BLK,)),
                pltpu.SemaphoreType.DMA,
                pltpu.SemaphoreType.DMA((4,)),
            ],
            compiler_params=pltpu.CompilerParams(collective_id=0, has_side_effects=True, vmem_limit_bytes=60 * 1024 * 1024),
        )(flat, jnp.asarray(cos_np), jnp.asarray(sin_np), *gain_vecs, *weights)
        return out[0].reshape(tokens.shape)

    mapped = jax.shard_map(local_fn, mesh=mesh, in_specs=(P(('dp', 'fsdp')), P(None, 'fsdp'), P(None, 'fsdp')), out_specs=P(('dp', 'fsdp')), check_vma=False)

    def run(tokens, w_query, w_key, w_value, w_out, w_gate, w_up, w_down, g_query, g_key, g_attn, g_mlp):
        return mapped(tokens, (w_query, w_key, w_value, w_out, w_gate, w_up, w_down), (g_query, g_key, g_attn, g_mlp))

    return run
```

```python
import functools

import jax
import jax.numpy as jnp
import numpy as np
from jax import lax
from jax.experimental import pallas as pl
from jax.experimental.pallas import tpu as pltpu
from jax.sharding import PartitionSpec as P

HEAD_DIM = 128
EPS = 1e-6
THETA = 500000.0
SEQ = 256
D = 2048
ROWS = 512
N_BLK = 8
BLK = 256
TILE = 512
N_TILE = D // TILE
HALF = D // 2
RB = 32
SLOTS = 2
MESH = pl.DeviceIdType.MESH

START = 0.0
ONE_MIB = 22.5
PAIRED = range(2)
ROLES = range(3)
QUAD = range(4)
UNIT = ONE_MIB / 256
LAT = 2.5
PAIR = 4.0
FLOW = {'A': (176, 144, 64), 'B': (144, 176, 144), 'C': (144, 176, 144), 'Q': (128, 128, 128), 'H': (144, 128, 128), 'G': (176, 144, 144)}
VIA_X = {'A': 64}
DOWN = {'H': 176, 'G': 208}
FLOW = {k: (px, py, VIA_X.get(k, 0), dy, DOWN.get(k, 0)) for k, (px, py, dy) in FLOW.items()}
ITEMS = ['Q'] * 3 + ['A'] + ['H'] * 4 + ['B'] * 4 + ['G'] * 3 + ['C'] * 3
BACKLOG = 8.0
N_H = (4, 3)
COST = {'mm': 6.6, 'at': 4.5, 'h': 10.5, 'wgu': 7.5, 'wd': 11.0, 'fin': 1.5}
SCALE = {'Q': 0.5}
BOTH = dict(COST, mq=11.0, mm=11.0, nr=3.0)


def slots(nh=N_H):
    out = []
    for k in ROLES:
        out.append(('mq', k, 0, k, 2))
    for k in PAIRED:
        out.append(('nr', 0, 0, k, 2))
    attn = (0, 4 + nh[0])
    for s in PAIRED:
        for q in (1, 0):
            out.append(('at', 0, 0, q, s))
        out.append(('mm', 3, 0, 3, s))
    for j in range(nh[0]):
        for s in PAIRED:
            out.append(('h', 4 + j, 0, j, s))
    for s in PAIRED:
        out.append(('fin', 0, 0, 0, s))
    a1 = attn[1]
    h0 = a1 + 4
    for s in PAIRED:
        for k in ROLES:
            out.append(('mm', a1 + k, 1, k, s))
        for q in PAIRED:
            out.append(('at', 0, 1, q, s))
        out.append(('mm', a1 + 3, 1, 3, s))
    for s in PAIRED:
        for j in range(nh[1]):
            out.append(('h', h0 + j, 1, j, s))
    w0 = h0 + nh[1]
    out.append(('wgu', w0, 1, 0, 2))
    out.append(('wgu', w0 + 1, 1, 1, 2))
    out.append(('wd', w0 + 2, 1, 4, 2))
    for s in PAIRED:
        out.append(('fin', 0, 1, 0, s))
    return out


def schedule(thr=20.0, nh=N_H):
    sl = slots(nh)
    t = START
    free = dict.fromkeys('xyzp', START)
    arr = {}
    prog = []

    def send(link, dur, key):
        s = max(free[link], t)
        free[link] = s + dur
        arr[key] = free[link] + LAT

    todo_send = {}
    for i, f in enumerate(ITEMS):
        px, py, dx, dy, pn = FLOW[f]
        a, b = 'xy'

        def add(k, link, dur, *deps, i=i, f=f):
            todo_send[(k, i)] = (i, link, dur * SCALE.get(f, 1.0), [(d, i) for d in deps])

        add('X', a, px * UNIT)
        add('Y', b, py * UNIT)
        add('P0', 'p', PAIR)
        add('DY', b, dy * UNIT, 'X')
        if dx:
            add('DX', a, dx * UNIT, 'Y')
        if px < BLK:
            add('ZX', 'z', (BLK - px) * UNIT, 'X')
            add('P1', 'p', PAIR, 'X', 'ZX')
        else:
            add('P1', 'p', PAIR, 'X')
        add('ZY', 'z', (BLK - py) * UNIT, 'Y')
        add('P2', 'p', PAIR, 'Y', 'ZY')
        diag = ('DX', 'DY') if dx else ('DY',)
        add('ZD', 'z', (BLK - dx - dy) * UNIT, *diag)
        add('P3', 'p', PAIR, *(diag + ('ZD',)))
        if pn:
            add('N', b, pn * UNIT)
            add('Q0', 'p', PAIR)
            add('ZN', 'z', (BLK - pn) * UNIT, 'N')
            add('Q1', 'p', PAIR, 'N', 'ZN')
    for h in PAIRED:
        todo_send[('T', 0, h)] = (-2, 'x', ONE_MIB, [])
    limit = dict(x=thr, y=thr, z=thr, p=2 * PAIR)

    def needs(s):
        ty, it, la, ex, hf = s
        n = []
        if ty in ('mm', 'mq', 'h', 'wgu', 'wd'):
            n += [('P%d' % k, it) for k in QUAD]
        if ty == 'h':
            n += [('Q%d' % k, it) for k in PAIRED]
            n.append(('H', la, hf))
        if ty == 'mq':
            n += [('T', 0, q) for q in PAIRED]
        if ty == 'nr':
            n.append(('S', 0, ex))
        if ty == 'mm' and la == 0:
            n.append(('O', 0, hf))
        if ty == 'fin':
            n.append(('R', la, hf))
        return n

    def after(s):
        ty, it, la, ex, hf = s
        halves = [hf] if hf < 2 else [0, 1]
        if ty == 'mm' and ex < 3:
            return [('fin', la - 1, 0, hf)] if la else []
        if ty == 'mq':
            return [('nr', 0, ex - 1, 2)] if ex else []
        if ty == 'nr':
            return [('mq', 0, ex, 2)]
        if ty == 'at':
            return [('mm', la, k, hf) for k in ROLES] if la else [('mq', 0, 2, 2)] + [('nr', 0, k, 2) for k in PAIRED]
        if ty == 'mm':
            return [('at', la, q, hf) for q in PAIRED]
        if ty == 'h':
            return [('mm', la, 3, q) for q in halves] + ([('h', la, ex - 1, hf)] if ex else [])
        if ty == 'wgu':
            return [('mm', la, 3, q) for q in PAIRED]
        if ty == 'wd':
            return [('wgu', la, 0, 2), ('wgu', la, 1, 2)] + [('h', la, nh[1] - 1, q) for q in PAIRED]
        return [('h', la, nh[la] - 1, hf)] + ([('wd', la, 4, 2)] if la else [])

    done = set()
    todo = list(range(len(sl)))
    while todo:
        again = True
        while again:
            again = False
            ready = {}
            for key, (pri, link, dur, deps) in todo_send.items():
                if free[link] - t < limit[link] and all(arr.get(x, 1e9) <= t for x in deps):
                    if link not in ready or (pri, len(deps) == 0) < ready[link][0]:
                        ready[link] = ((pri, len(deps) == 0), key)
            for link, (_, key) in ready.items():
                send(link, todo_send[key][2], key)
                prog.append(('send', key, todo_send.pop(key)[3]))
                again = True
        pick = None
        ev = [arr[x] for e in todo_send.values() for x in e[3] if x in arr]
        ev += [free[e[1]] - limit[e[1]] + 0.01 for e in todo_send.values()]
        for k in todo:
            s = sl[k]
            if not all(x in done for x in after(s)):
                continue
            ns = needs(s)
            if all(arr.get(x, 1e9) <= t for x in ns):
                pick = k
                break
            ev += [arr[x] for x in ns if x in arr]
        if pick is not None:
            ty, it, la, ex, hf = sl[pick]
            todo.remove(pick)
            prog.append(('slot', pick))
            t += BOTH[ty] if hf not in PAIRED else COST[ty]
            done.add((ty, la, ex, hf))
            for q in [hf] if hf in PAIRED else PAIRED:
                key = None
                if ty == 'mq' and ex in PAIRED and not q:
                    key, units = ('S', 0, ex), 0.05
                if ty == 'at' and not la and ex:
                    key, units = ('O', 0, hf), 0.5
                if ty == 'mm' and ex == 3:
                    key, units = ('H', la, q), 1
                if ty == 'h' and ex == nh[la] - 1:
                    key, units = ('R', la, q), 2
                if key:
                    todo_send[key] = (-1, 'x', units * ONE_MIB, [])
            continue
        t = min(e for e in ev if e > t)
    assert not todo_send
    return sl, prog, t


def plan():
    sl, prog, _ = schedule(BACKLOG, N_H)
    order, lists, cur, seen = [], [], [], set()

    def await_all(keys):
        for key in keys:
            if key not in seen:
                seen.add(key)
                cur.append(('wait', key))

    for op in prog:
        if op[0] == 'send':
            await_all(op[2])
            cur.append(('send', op[1]))
            continue
        s = sl[op[1]]
        ty, it, la, ex, hf = s
        if ty in ('mm', 'mq', 'h', 'wgu', 'wd'):
            await_all([('P%d' % k, it) for k in QUAD])
        if ty == 'h':
            await_all([('Q%d' % k, it) for k in PAIRED])
            await_all([('H', la, hf)])
            if la == 1 and ex == 0:
                cur.append(('drain', ('R', 0, hf)))
        if ty == 'mq':
            await_all([('T', 0, q) for q in PAIRED])
        if ty == 'nr':
            await_all([('S', 0, ex)])
        if ty == 'mm' and la == 0:
            await_all([('O', 0, hf)])
        if ty == 'mm' and la == 1 and ex == 0:
            cur.append(('drain', ('O', 0, hf)))
        if ty == 'fin':
            await_all([('R', la, hf)])
        order.append(s)
        lists.append(cur)
        cur = []
    assert not cur and all(k in seen for k, _ in KEYS)
    return order, lists


def copy_keys():
    keys = []
    for i, f in enumerate(ITEMS):
        px, py, dx, dy, pn = FLOW[f]
        rows = {'X': px, 'Y': py, 'P0': BLK, 'DX': dx, 'DY': dy, 'ZX': BLK - px, 'ZY': BLK - py, 'ZD': BLK - dx - dy, 'P1': BLK, 'P2': BLK, 'P3': BLK}
        if pn:
            rows.update({'N': pn, 'ZN': BLK - pn, 'Q0': BLK, 'Q1': BLK})
        keys += [((k, i), r) for k, r in rows.items() if r]
    for s in PAIRED:
        keys += [(('T', 0, s), BLK), (('S', 0, s), 0), (('O', 0, s), BLK)]
    for la in PAIRED:
        for s in PAIRED:
            keys += [(('H', la, s), BLK), (('R', la, s), 0)]
    return keys


KEYS = copy_keys()
SID = {k: n for n, (k, _) in enumerate(KEYS)}
KROWS = dict(KEYS)
H_ITEMS = [i for i, f in enumerate(ITEMS) if FLOW[f][4]]
ATTN0 = (0, 4 + N_H[0])
W_ITEM = 8 + N_H[0] + N_H[1]


def shared_col(n, side, j):
    return 4096 * (n // 2) + 2048 * side + 1024 * (n % 2) + BLK * j


def head(h):
    return slice(h * HEAD_DIM, (h + 1) * HEAD_DIM)


def tile(n):
    return slice(n * TILE, (n + 1) * TILE)


def seq(s):
    return pl.ds(pl.multiple_of(s * SEQ, SEQ), SEQ)


def loop(n, body):
    lax.fori_loop(0, n, body, 0)


def rope_tables():
    pos = np.arange(SEQ, dtype=np.float64)
    inv = THETA ** (-2.0 * np.arange(HEAD_DIM // 2, dtype=np.float64) / HEAD_DIM)
    ang = pos[:, None] * inv[None, :]
    cos, sin = np.cos(ang), np.sin(ang)
    return (np.concatenate([cos, cos], 1).astype(np.float32), np.concatenate([-sin, sin], 1).astype(np.float32))


def width(key):
    narrow = key[0] == 'O' or (len(key) == 2 and ITEMS[key[1]] == 'Q')
    return HALF if narrow else D


def kernel(x_hbm, cos_ref, sin_ref, gq, gk, ga, gm, wq, wk, wv, wo, wg, wu, wd, out_hbm, full, full_n, act, h2, mj, acc, rs, xo, st_out, st_in, wt, gains, gain_in, gain_ref, send_sem, recv_sem, wt_sem, gs_sem, gr_sem, io_sem, gi_sem):
    zz = lax.axis_index('dp')
    me = lax.axis_index('fsdp')
    cc = me % 2
    xx = (me // 2) % 2
    yy = me // 4

    def at(y, x, c):
        return y * 4 + x * 2 + c

    f_p = at(yy, xx, 1 - cc)
    f_x = at(yy, 1 - xx, cc)
    f_y = at(1 - yy, xx, cc)
    f_d = at(1 - yy, 1 - xx, cc)
    n_me, n_y = yy * 2 + cc, (1 - yy) * 2 + cc
    dev_p, dev_x, dev_y, dev_z = (zz, f_p), (zz, f_x), (zz, f_y), (1 - zz, me)

    x_copy = pltpu.make_async_copy(x_hbm, act.at[0], io_sem)
    x_copy.start()

    gain_loads = [pltpu.make_async_copy(g, gain_in.at[k], gi_sem.at[k]) for k, g in enumerate((gq, gk, ga, gm))]
    for cp in gain_loads:
        cp.start()
    for k, cp in enumerate(gain_loads):
        cp.wait()
        for la in PAIRED:
            gain_ref[la * 4 + k:la * 4 + k + 1, :] = gain_in[k, la:la + 1, :].astype(jnp.float32)

    barrier = pltpu.get_barrier_semaphore()
    for k in range(1, N_BLK):
        pl.semaphore_signal(barrier, inc=1, device_id=(zz, (me + k) % N_BLK), device_id_type=MESH)
    pl.semaphore_signal(barrier, inc=1, device_id=dev_z, device_id_type=MESH)
    pl.semaphore_wait(barrier, N_BLK)

    def m16(v):
        return pl.multiple_of(v, 16)

    def m256(v):
        return pl.multiple_of(v, 256)

    def remote(key, src, dst, dev):
        return pltpu.make_async_remote_copy(src, dst, send_sem.at[SID[key]], recv_sem.at[SID[key]], device_id=dev, device_id_type=MESH)

    def same_size(key):
        if key[0] == 'R':
            piece = rs.at[0, 0]
        elif key[0] == 'S':
            piece = st_in.at[key[2]]
        else:
            piece = full.at[0, 0, pl.ds(0, KROWS[key]), pl.ds(0, width(key))]
        return remote(key, piece, piece, dev_p)

    def arrived(key):
        same_size(key).wait_recv()

    def own_pieces(i, side):
        la = int(i >= ATTN0[1])
        if i >= W_ITEM:
            if i == W_ITEM + 2:
                return [(wd.at[la, pl.ds(3 * BLK, BLK), :], 0, D)]
            cols = [1024 * (4 * (i - W_ITEM) + n) + 3 * BLK for n in QUAD]
        elif i in H_ITEMS:
            j = i - ATTN0[la] - 4
            cols = [m256(shared_col(n, side, j)) for n in QUAD]
        elif ITEMS[i] == 'Q':
            return [((wq, wk, wv)[i].at[0, :, pl.ds(m256(HALF * side), HALF)], 0, HALF)]
        else:
            return [((wq, wk, wv, wo)[i - ATTN0[la]].at[la], 0, D)]
        out = []
        for n, c in enumerate(cols):
            out.append((wg.at[la, :, pl.ds(c, BLK)], n * TILE, BLK))
            out.append((wu.at[la, :, pl.ds(c, BLK)], n * TILE + BLK, BLK))
        return out

    def send_own(key, side, off, dev):
        i = key[1]
        part = pl.ds(off, KROWS[key])
        for src, c0, nc in own_pieces(i, side):
            remote(key, src.at[part, :], full.at[i, me, part, pl.ds(c0, nc)], dev).start()

    def push(key, blk, off, dev):
        piece = full.at[key[1], blk, pl.ds(off, KROWS[key]), pl.ds(0, width(key))]
        remote(key, piece, piece, dev).start()

    def push_n(key, off, dev):
        piece = full_n.at[H_ITEMS.index(key[1]), n_y, pl.ds(off, KROWS[key]), :]
        remote(key, piece, piece, dev).start()

    def own_n(key, off, dev):
        i = key[1]
        la = int(i >= ATTN0[1])
        r0 = BLK * (i - ATTN0[la] - 4)
        rr = KROWS[key]
        remote(key, wd.at[la, pl.ds(m16(r0 + off), rr), :], full_n.at[H_ITEMS.index(i), n_me, pl.ds(off, rr), :], dev).start()

    def transfer(op):
        key = op[1]
        if op[0] == 'wait':
            return arrived(key)
        if op[0] == 'drain':
            return same_size(key).wait_send()
        kind = key[0]
        if kind == 'T':
            return remote(key, x_hbm.at[pl.ds(key[2] * SEQ, SEQ), :], xo.at[key[2]], dev_x).start()
        if kind == 'S':
            return remote(key, st_out.at[key[2]], st_in.at[key[2]], dev_x).start()
        if kind == 'O':
            sq = pl.ds(key[2] * SEQ, SEQ)
            return remote(key, act.at[1, sq, pl.ds(HALF, HALF)], act.at[4, sq, pl.ds(m256(HALF * xx), HALF)], dev_x).start()
        if kind == 'H':
            la, s = key[1:]
            return remote(key, h2.at[la, s, pl.ds(0, SEQ), :], h2.at[la, s, pl.ds(SEQ, SEQ), :], dev_x).start()
        if kind == 'R':
            la, s = key[1:]
            return remote(key, acc.at[s, pl.ds(SEQ, SEQ), :], rs.at[la, s], dev_x).start()
        px, py, dx, dy, pn = FLOW[ITEMS[key[1]]]
        off_d = m16((BLK - dx - dy) * zz)
        steps = {
            'X': lambda: send_own(key, 1 - xx, m16((BLK - px) * zz), dev_x),
            'Y': lambda: send_own(key, xx, m16((BLK - py) * zz), dev_y),
            'P0': lambda: send_own(key, xx, 0, dev_p),
            'ZX': lambda: push(key, f_x, m16(px * zz), dev_z),
            'ZY': lambda: push(key, f_y, m16(py * zz), dev_z),
            'ZD': lambda: push(key, f_d, m16((dx + dy) * zz), dev_z),
            'DX': lambda: push(key, f_y, off_d, dev_x),
            'DY': lambda: push(key, f_x, m16(off_d + dx), dev_y),
            'P1': lambda: push(key, f_x, 0, dev_p),
            'P2': lambda: push(key, f_y, 0, dev_p),
            'P3': lambda: push(key, f_d, 0, dev_p),
            'N': lambda: own_n(key, m16((BLK - pn) * zz), dev_y),
            'Q0': lambda: own_n(key, 0, dev_p),
            'ZN': lambda: push_n(key, m16(pn * zz), dev_z),
            'Q1': lambda: push_n(key, 0, dev_p),
        }
        steps[kind]()

    order, lists = plan()
    n_slot = len(order)

    def load(parts, slot):
        for src, dst in parts:
            pltpu.make_async_copy(src, dst, wt_sem.at[slot]).start()

    def others(i, n):
        slot = n % SLOTS
        cols = pl.ds(n * TILE, TILE)
        load([(full.at[i, (me + k) % N_BLK, :, cols], wt.at[slot, (me + k) % N_BLK]) for k in range(1, N_BLK)], slot)

    def wait_tile(n, blocks=N_BLK):
        slot = n % SLOTS
        part = wt.at[slot, pl.ds(0, blocks)]
        pltpu.make_async_copy(full.at[0, pl.ds(0, blocks), :, pl.ds(0, TILE)], part, wt_sem.at[slot]).wait()

    def load_mm(i, la, role, n):
        slot = n % SLOTS
        cols = pl.ds(n * TILE, TILE)
        for k, w in enumerate((wq, wk, wv, wo)):
            pl.when(role == k)(functools.partial(load, [(w.at[la, :, cols], wt.at[slot, me])], slot))
        pl.when(role == 4)(functools.partial(load, [(wd.at[1, pl.ds(3 * BLK, BLK), cols], wt.at[slot, me])], slot))
        others(i, n)

    def load_gu(i, la, col, n):
        slot = n % SLOTS
        c = pl.ds(m256(col(n)), BLK)
        load([(wg.at[la, :, c], wt.at[slot, me, :, pl.ds(0, BLK)]), (wu.at[la, :, c], wt.at[slot, me, :, pl.ds(BLK, BLK)])], slot)
        others(i, n)

    def load_dn(hn, la, j, n):
        slot = n % SLOTS
        cols = pl.ds(n * TILE, TILE)
        parts = [(wd.at[la, pl.ds(m256(j * BLK), BLK), cols], wt.at[slot, n_me])]
        parts += [(full_n.at[hn, (n_me + k) % 4, :, cols], wt.at[slot, (n_me + k) % 4]) for k in range(1, 4)]
        load(parts, slot)

    def gain_row(la, k):
        return jnp.concatenate([gains[f, pl.ds(la * 4 + k, 1), :] for f in range(N_BLK)], axis=1)

    def scaled(v, gain):
        a = v.astype(jnp.bfloat16).astype(jnp.float32)
        ms = jnp.mean(a * a, axis=-1, keepdims=True)
        return a * lax.rsqrt(ms + EPS) * gain

    def rows(body):
        def step(r, carry):
            body(pl.multiple_of(r * RB, RB))
            return carry

        loop(SEQ // RB, step)

    def act_rows(s, r0):
        return pl.ds(pl.multiple_of(s * SEQ + r0, RB), RB)

    def norm_rope(la, k, dst, s):
        gain = gain_row(la, k)

        def body(r0):
            v = scaled(acc[s, pl.ds(r0, RB), :], gain)
            c = cos_ref[pl.ds(r0, RB), :]
            sn = sin_ref[pl.ds(r0, RB), :]
            for h in range(D // HEAD_DIM):
                part = v[:, head(h)]
                turned = pltpu.roll(part, HEAD_DIM // 2, 1)
                act[dst, act_rows(s, r0), head(h)] = (part * c + turned * sn).astype(jnp.bfloat16)

        rows(body)

    def attention(q8, la, s):
        split = (la == 0) & (q8 == 0)
        dst = jnp.where(split, 4, 1)
        base = jnp.where(split, xx * (HALF), q8 * (HALF))
        row = lax.broadcasted_iota(jnp.int32, (SEQ, SEQ), 0)
        col = lax.broadcasted_iota(jnp.int32, (SEQ, SEQ), 1)
        causal = row >= col
        sq = seq(s)

        def step(h, carry):
            for u in PAIRED:
                lanes = pl.ds(pl.multiple_of((q8 * 8 + h * 2 + u) * HEAD_DIM, HEAD_DIM), HEAD_DIM)
                q, k, v = act[1, sq, lanes], act[2, sq, lanes], act[3, sq, lanes]
                sc = lax.dot_general(q, k, (((1,), (1,)), ((), ())), preferred_element_type=jnp.float32) * (HEAD_DIM ** -0.5)
                sc = jnp.where(causal, sc, -jnp.inf)
                e = jnp.exp(sc - jnp.max(sc, axis=-1, keepdims=True))
                p = (e / jnp.sum(e, axis=-1, keepdims=True)).astype(jnp.bfloat16)
                out = pl.ds(pl.multiple_of(base + (h * 2 + u) * HEAD_DIM, HEAD_DIM), HEAD_DIM)
                act[dst, sq, out] = jnp.dot(p, v, preferred_element_type=jnp.float32).astype(jnp.bfloat16)
            return carry

        loop(4, step)

    def mm(i, la, role, hf):
        s0 = jnp.where(hf == 2, 0, hf)
        s1 = jnp.where(hf == 2, 2, hf + 1)
        lhs = jnp.where(role < 3, 0, jnp.where((role == 3) & (la == 1), 1, 4))
        load_mm(i, la, role, 0)
        for n in range(N_TILE):
            if n + 1 < N_TILE:
                load_mm(i, la, role, n + 1)
            wait_tile(n)
            cols = tile(n)

            def one(s, carry):
                left = act[lhs, seq(s), :]
                prod = jnp.dot(left, wt[n % SLOTS].reshape(D, TILE), preferred_element_type=jnp.float32)
                acc[s, :SEQ, cols] = jnp.where(role == 4, acc[s, :SEQ, cols], 0.0) + prod
                return carry

            lax.fori_loop(s0, s1, one, 0)

        def epilogue(s, carry):
            @pl.when(role == 0)
            def _():
                norm_rope(la, 0, 1, s)

            @pl.when(role == 1)
            def _():
                norm_rope(la, 1, 2, s)

            @pl.when(role == 2)
            def _():
                def body(r0):
                    act[3, act_rows(s, r0), :] = acc[s, pl.ds(r0, RB), :].astype(jnp.bfloat16)

                rows(body)

            @pl.when(role == 3)
            def _():
                gain = gain_row(la, 2)

                def body(r0):
                    h = act[0, act_rows(s, r0), :].astype(jnp.float32) + scaled(acc[s, pl.ds(r0, RB), :], gain)
                    h2[la, s, pl.ds(r0, RB), :] = h.astype(jnp.bfloat16)

                rows(body)

            return carry

        lax.fori_loop(s0, s1, epilogue, 0)

    def load_mq(k, n):
        slot = n % SLOTS
        for r, w in enumerate((wq, wk, wv)):
            own = w.at[0, :, pl.ds(m256(HALF * xx + n * TILE), TILE)]
            pl.when(k == r)(functools.partial(load, [(own, wt.at[slot, me])], slot))
        others(k, n)

    def shared_qkv(k):
        load_mq(k, 0)
        for n in PAIRED:
            if n == 0:
                load_mq(k, 1)
            wait_tile(n)
            cols = tile(n)

            def one(s, carry):
                w = wt[n % SLOTS].reshape(D, TILE)
                sq = seq(s)
                acc[s, :SEQ, cols] = jnp.dot(act[0, sq, :], w, preferred_element_type=jnp.float32)
                acc[s, SEQ:, cols] = jnp.dot(xo[s], w, preferred_element_type=jnp.float32)
                return carry

            loop(2, one)

        @pl.when(k == 2)
        def _():
            def keep(s, carry):
                for part in PAIRED:
                    def body(r0, part=part):
                        v = acc[s, pl.ds(part * SEQ + r0, RB), :HALF]
                        act[3, act_rows(s, r0), part * (HALF):(part + 1) * (HALF)] = v.astype(jnp.bfloat16)

                    rows(body)
                return carry

            loop(2, keep)

        @pl.when(k < 2)
        def _():
            def squares(s, carry):
                for part in PAIRED:
                    for r in PAIRED:
                        r0 = part * SEQ + r * HEAD_DIM
                        total = jnp.zeros((HEAD_DIM, HEAD_DIM), jnp.float32)
                        for h in range(8):
                            a = acc[s, r0:r0 + HEAD_DIM, head(h)].astype(jnp.bfloat16).astype(jnp.float32)
                            total = total + a * a
                        col = jnp.broadcast_to(jnp.sum(total, axis=-1, keepdims=True), (HEAD_DIM, HEAD_DIM))
                        st_out[k, s * 2 + part, :, head(r)] = col.T[:8, :]
                return carry

            loop(2, squares)

    def shared_rope(k):
        gain = jnp.concatenate([gains[xx * 4 + f, pl.ds(k, 1), :] for f in QUAD], axis=1)

        def one(s, carry):
            for part in PAIRED:
                for r in PAIRED:
                    lanes = head(r)
                    sums = st_out[k, s * 2 + part, :, lanes] + st_in[k, s * 2 + 1 - part, :, lanes]
                    col = jnp.broadcast_to(sums[:1, :], (HEAD_DIM, HEAD_DIM)).T
                    inv = lax.rsqrt(col * (1.0 / D) + EPS)
                    c, sn = cos_ref[lanes, :], sin_ref[lanes, :]
                    r0 = part * SEQ + r * HEAD_DIM
                    rr = pl.ds(pl.multiple_of(s * SEQ + r * HEAD_DIM, HEAD_DIM), HEAD_DIM)
                    for h in range(8):
                        hs = head(h)
                        a = acc[s, r0:r0 + HEAD_DIM, hs].astype(jnp.bfloat16).astype(jnp.float32)
                        v = a * inv * gain[:, hs]
                        turned = pltpu.roll(v, HEAD_DIM // 2, 1)
                        o0 = part * (HALF) + h * HEAD_DIM
                        act[k + 1, rr, o0:o0 + HEAD_DIM] = (v * c + turned * sn).astype(jnp.bfloat16)
            return carry

        loop(2, one)

    def swiglu(prod):
        gate = prod[:, :BLK].astype(jnp.bfloat16).astype(jnp.float32)
        up = prod[:, BLK:].astype(jnp.bfloat16).astype(jnp.float32)
        return (jax.nn.silu(gate) * up).astype(jnp.bfloat16)

    def shared_mlp(i, hn, la, j, s):
        def col(n):
            return shared_col(n, xx, j)

        load_gu(i, la, col, 0)
        for n in range(N_TILE):
            if n + 1 < N_TILE:
                load_gu(i, la, col, n + 1)
            else:
                load_dn(hn, la, j, 0)
            wait_tile(n)
            prod = jnp.dot(h2[la, s], wt[n % SLOTS].reshape(D, TILE), preferred_element_type=jnp.float32)
            mj[:, n * BLK:(n + 1) * BLK] = swiglu(prod)
        for n in range(N_TILE):
            if n + 1 < N_TILE:
                load_dn(hn, la, j, n + 1)
            wait_tile(n, 4)
            cols = tile(n)
            prod = jnp.dot(mj[...], wt[n % SLOTS, :4].reshape(4 * BLK, TILE), preferred_element_type=jnp.float32)
            acc[s, :, cols] = jnp.where(j > 0, acc[s, :, cols], 0.0) + prod

    def plain_gu(i, e):
        def col(n):
            return 1024 * (4 * e + n) + 3 * BLK

        load_gu(i, 1, col, 0)
        for n in range(N_TILE):
            if n + 1 < N_TILE:
                load_gu(i, 1, col, n + 1)
            wait_tile(n)

            def one(s, carry):
                prod = jnp.dot(h2[1, s, :SEQ], wt[n % SLOTS].reshape(D, TILE), preferred_element_type=jnp.float32)
                act[4, seq(s), pl.ds(m256(e * 1024 + n * BLK), BLK)] = swiglu(prod)
                return carry

            loop(2, one)

    def finish(la, s):
        gain = gain_row(la, 3)

        def body(r0):
            y = scaled(acc[s, pl.ds(r0, RB), :] + rs[la, s, pl.ds(r0, RB), :], gain)
            act[0, act_rows(s, r0), :] = (h2[la, s, pl.ds(r0, RB), :].astype(jnp.float32) + y).astype(jnp.bfloat16)

        rows(body)

    def pick(p, values):
        out = jnp.int32(0)
        for k, v in enumerate(values):
            if v:
                out = jnp.where(p == k, v, out)
        return out

    gain_copies = []
    for k in range(1, N_BLK):
        cp = pltpu.make_async_remote_copy(gain_ref, gains.at[me], gs_sem.at[k], gr_sem.at[k], device_id=(zz, (me + k) % N_BLK), device_id_type=MESH)
        gain_copies.append(cp)

    types = ['mm', 'at', 'h', 'wgu', 'wd', 'fin', 'mq', 'nr']

    def step(p, carry):
        for k in range(n_slot):
            if not lists[k]:
                continue

            @pl.when(p == k)
            def _(k=k):
                if k == 0:
                    for cp in gain_copies:
                        cp.start()
                for op in lists[k]:
                    transfer(op)
                if k == 0:
                    x_copy.wait()
                    for cp in gain_copies:
                        cp.wait()
                    gains[pl.ds(me, 1)] = gain_ref[...][None]

        ty = pick(p, [types.index(o[0]) for o in order])
        item = pick(p, [o[1] for o in order])
        la = pick(p, [o[2] for o in order])
        ex = pick(p, [o[3] for o in order])
        hf = pick(p, [o[4] for o in order])
        hn = pick(p, [H_ITEMS.index(o[1]) if o[0] == 'h' else 0 for o in order])
        pl.when((ty == 0) | (ty == 4))(lambda: mm(item, la, ex, hf))
        pl.when(ty == 1)(lambda: attention(ex, la, hf))
        pl.when(ty == 2)(lambda: shared_mlp(item, hn, la, ex, hf))
        pl.when(ty == 3)(lambda: plain_gu(item, ex))
        pl.when(ty == 5)(lambda: finish(la, hf))
        pl.when(ty == 6)(lambda: shared_qkv(ex))
        pl.when(ty == 7)(lambda: shared_rope(ex))
        return carry

    loop(n_slot, step)

    out_copy = pltpu.make_async_copy(act.at[0], out_hbm, io_sem)
    out_copy.start()
    drained = [op[1] for ops in lists for op in ops if op[0] == 'drain']
    for key, _ in KEYS:
        if key not in drained:
            same_size(key).wait_send()
    out_copy.wait()


def solution(mesh):
    cos_np, sin_np = rope_tables()
    hbm = pl.BlockSpec(memory_space=pl.ANY)
    vmem = pl.BlockSpec(memory_space=pltpu.VMEM)
    n_copy = len(KEYS)

    def local_fn(tokens, weights, gain_vecs):
        flat = tokens.reshape(ROWS, D)
        out = pl.pallas_call(
            kernel,
            out_shape=(
                jax.ShapeDtypeStruct((ROWS, D), jnp.bfloat16),
                jax.ShapeDtypeStruct((len(ITEMS), N_BLK, BLK, D), jnp.bfloat16),
                jax.ShapeDtypeStruct((len(H_ITEMS), 4, BLK, D), jnp.bfloat16),
            ),
            in_specs=[hbm, vmem, vmem] + [hbm] * 11,
            out_specs=(hbm, hbm, hbm),
            scratch_shapes=[
                pltpu.VMEM((5, ROWS, D), jnp.bfloat16),
                pltpu.VMEM((2, 2, 2 * SEQ, D), jnp.bfloat16),
                pltpu.VMEM((2 * SEQ, 4 * BLK), jnp.bfloat16),
                pltpu.VMEM((2, 2 * SEQ, D), jnp.float32),
                pltpu.VMEM((2, 2, SEQ, D), jnp.float32),
                pltpu.VMEM((2, SEQ, D), jnp.bfloat16),
                pltpu.VMEM((2, 4, 8, SEQ), jnp.float32),
                pltpu.VMEM((2, 4, 8, SEQ), jnp.float32),
                pltpu.VMEM((2, N_BLK, BLK, TILE), jnp.bfloat16),
                pltpu.VMEM((N_BLK, 8, BLK), jnp.float32),
                pltpu.VMEM((4, 2, BLK), jnp.bfloat16),
                pltpu.VMEM((8, BLK), jnp.float32),
                pltpu.SemaphoreType.DMA((n_copy,)),
                pltpu.SemaphoreType.DMA((n_copy,)),
                pltpu.SemaphoreType.DMA((2,)),
                pltpu.SemaphoreType.DMA((N_BLK,)),
                pltpu.SemaphoreType.DMA((N_BLK,)),
                pltpu.SemaphoreType.DMA,
                pltpu.SemaphoreType.DMA((4,)),
            ],
            compiler_params=pltpu.CompilerParams(collective_id=0, has_side_effects=True, vmem_limit_bytes=60 * 1024 * 1024),
        )(flat, jnp.asarray(cos_np), jnp.asarray(sin_np), *gain_vecs, *weights)
        return out[0].reshape(tokens.shape)

    mapped = jax.shard_map(local_fn, mesh=mesh, in_specs=(P(('dp', 'fsdp')), P(None, 'fsdp'), P(None, 'fsdp')), out_specs=P(('dp', 'fsdp')), check_vma=False)

    def run(tokens, w_query, w_key, w_value, w_out, w_gate, w_up, w_down, g_query, g_key, g_attn, g_mlp):
        return mapped(tokens, (w_query, w_key, w_value, w_out, w_gate, w_up, w_down), (g_query, g_key, g_attn, g_mlp))

    return run
```

```python
import functools

import jax
import jax.numpy as jnp
import numpy as np
from jax import lax
from jax.experimental import pallas as pl
from jax.experimental.pallas import tpu as pltpu
from jax.sharding import PartitionSpec as P

HEAD_DIM = 128
EPS = 1e-6
THETA = 500000.0
SEQ = 256
D = 2048
ROWS = 512
N_BLK = 8
BLK = 256
TILE = 512
N_TILE = D // TILE
HALF = D // 2
RB = 32
SLOTS = 2
MESH = pl.DeviceIdType.MESH

START = 0.0
ONE_MIB = 22.5
PAIRED = range(2)
ROLES = range(3)
QUAD = range(4)
UNIT = ONE_MIB / 256
LAT = 2.5
PAIR = 4.0
FLOW = {'A': (176, 128, 16), 'B': (144, 160, 128), 'C': (144, 176, 128), 'Q': (144, 128, 128), 'H': (176, 128, 128), 'G': (128, 192, 128)}
VIA_X = {'A': 112}
DOWN = {'H': 160, 'G': 208}
FLOW = {k: (px, py, VIA_X.get(k, 0), dy, DOWN.get(k, 0)) for k, (px, py, dy) in FLOW.items()}
ITEMS = ['Q'] * 3 + ['A'] + ['H'] * 4 + ['B'] * 4 + ['G'] * 3 + ['C'] * 3
BACKLOG = 10.0
N_H = (4, 3)
COST = {'mm': 6.6, 'at': 4.5, 'h': 10.5, 'wgu': 7.5, 'wd': 11.0, 'fin': 1.5}
SCALE = {'Q': 0.5}
BOTH = dict(COST, mq=11.0, mm=11.0, nr=3.0)


def slots(nh=N_H):
    out = []
    for k in ROLES:
        out.append(('mq', k, 0, k, 2))
    for k in PAIRED:
        out.append(('nr', 0, 0, k, 2))
    attn = (0, 4 + nh[0])
    for s in PAIRED:
        for q in (1, 0):
            out.append(('at', 0, 0, q, s))
        out.append(('mm', 3, 0, 3, s))
    for j in range(nh[0]):
        for s in PAIRED:
            out.append(('h', 4 + j, 0, j, s))
    for s in PAIRED:
        out.append(('fin', 0, 0, 0, s))
    a1 = attn[1]
    h0 = a1 + 4
    for s in PAIRED:
        for k in ROLES:
            out.append(('mm', a1 + k, 1, k, s))
        for q in PAIRED:
            out.append(('at', 0, 1, q, s))
        out.append(('mm', a1 + 3, 1, 3, s))
    for s in PAIRED:
        for j in range(nh[1]):
            out.append(('h', h0 + j, 1, j, s))
    w0 = h0 + nh[1]
    out.append(('wgu', w0, 1, 0, 2))
    out.append(('wgu', w0 + 1, 1, 1, 2))
    out.append(('wd', w0 + 2, 1, 4, 2))
    for s in PAIRED:
        out.append(('fin', 0, 1, 0, s))
    return out


def schedule(thr=20.0, nh=N_H):
    sl = slots(nh)
    t = START
    free = dict.fromkeys('xyzp', START)
    arr = {}
    prog = []

    def send(link, dur, key):
        s = max(free[link], t)
        free[link] = s + dur
        arr[key] = free[link] + LAT

    todo_send = {}
    for i, f in enumerate(ITEMS):
        px, py, dx, dy, pn = FLOW[f]
        a, b = 'xy'

        def add(k, link, dur, *deps, i=i, f=f):
            todo_send[(k, i)] = (i, link, dur * SCALE.get(f, 1.0), [(d, i) for d in deps])

        add('X', a, px * UNIT)
        add('Y', b, py * UNIT)
        add('P0', 'p', PAIR)
        add('DY', b, dy * UNIT, 'X')
        if dx:
            add('DX', a, dx * UNIT, 'Y')
        if px < BLK:
            add('ZX', 'z', (BLK - px) * UNIT, 'X')
            add('P1', 'p', PAIR, 'X', 'ZX')
        else:
            add('P1', 'p', PAIR, 'X')
        add('ZY', 'z', (BLK - py) * UNIT, 'Y')
        add('P2', 'p', PAIR, 'Y', 'ZY')
        diag = ('DX', 'DY') if dx else ('DY',)
        add('ZD', 'z', (BLK - dx - dy) * UNIT, *diag)
        add('P3', 'p', PAIR, *(diag + ('ZD',)))
        if pn:
            add('N', b, pn * UNIT)
            add('Q0', 'p', PAIR)
            add('ZN', 'z', (BLK - pn) * UNIT, 'N')
            add('Q1', 'p', PAIR, 'N', 'ZN')
    for h in PAIRED:
        todo_send[('T', 0, h)] = (0.5, 'x', ONE_MIB, [])
    limit = dict(x=thr, y=thr, z=thr, p=2 * PAIR)

    def needs(s):
        ty, it, la, ex, hf = s
        n = []
        if ty in ('mm', 'mq', 'h', 'wgu', 'wd'):
            n += [('P%d' % k, it) for k in QUAD]
        if ty == 'h':
            n += [('Q%d' % k, it) for k in PAIRED]
            n.append(('H', la, hf))
        if ty == 'mq':
            n += [('T', 0, q) for q in PAIRED]
        if ty == 'nr':
            n.append(('S', 0, ex))
        if ty == 'mm' and la == 0:
            n.append(('O', 0, hf))
        if ty == 'fin':
            n.append(('R', la, hf))
        return n

    def after(s):
        ty, it, la, ex, hf = s
        halves = [hf] if hf < 2 else [0, 1]
        if ty == 'mm' and ex < 3:
            return [('fin', la - 1, 0, hf)] if la else []
        if ty == 'mq':
            return [('nr', 0, ex - 1, 2)] if ex else []
        if ty == 'nr':
            return [('mq', 0, ex, 2)]
        if ty == 'at':
            return [('mm', la, k, hf) for k in ROLES] if la else [('mq', 0, 2, 2)] + [('nr', 0, k, 2) for k in PAIRED]
        if ty == 'mm':
            return [('at', la, q, hf) for q in PAIRED]
        if ty == 'h':
            return [('mm', la, 3, q) for q in halves] + ([('h', la, ex - 1, hf)] if ex else [])
        if ty == 'wgu':
            return [('mm', la, 3, q) for q in PAIRED]
        if ty == 'wd':
            return [('wgu', la, 0, 2), ('wgu', la, 1, 2)] + [('h', la, nh[1] - 1, q) for q in PAIRED]
        return [('h', la, nh[la] - 1, hf)] + ([('wd', la, 4, 2)] if la else [])

    done = set()
    todo = list(range(len(sl)))
    while todo:
        again = True
        while again:
            again = False
            ready = {}
            for key, (pri, link, dur, deps) in todo_send.items():
                if free[link] - t < limit[link] and all(arr.get(x, 1e9) <= t for x in deps):
                    if link not in ready or (pri, len(deps) == 0) < ready[link][0]:
                        ready[link] = ((pri, len(deps) == 0), key)
            for link, (_, key) in ready.items():
                send(link, todo_send[key][2], key)
                prog.append(('send', key, todo_send.pop(key)[3]))
                again = True
        pick = None
        ev = [arr[x] for e in todo_send.values() for x in e[3] if x in arr]
        ev += [free[e[1]] - limit[e[1]] + 0.01 for e in todo_send.values()]
        for k in todo:
            s = sl[k]
            if not all(x in done for x in after(s)):
                continue
            ns = needs(s)
            if all(arr.get(x, 1e9) <= t for x in ns):
                pick = k
                break
            ev += [arr[x] for x in ns if x in arr]
        if pick is not None:
            ty, it, la, ex, hf = sl[pick]
            todo.remove(pick)
            prog.append(('slot', pick))
            t += BOTH[ty] if hf not in PAIRED else COST[ty]
            done.add((ty, la, ex, hf))
            for q in [hf] if hf in PAIRED else PAIRED:
                key = None
                if ty == 'mq' and ex in PAIRED and not q:
                    key, units = ('S', 0, ex), 0.05
                if ty == 'at' and not la and ex:
                    key, units = ('O', 0, hf), 0.5
                if ty == 'mm' and ex == 3:
                    key, units = ('H', la, q), 1
                if ty == 'h' and ex == nh[la] - 1:
                    key, units = ('R', la, q), 2
                if key:
                    todo_send[key] = (-1, 'x', units * ONE_MIB, [])
            continue
        t = min(e for e in ev if e > t)
    assert not todo_send
    return sl, prog, t


def plan():
    sl, prog, _ = schedule(BACKLOG, N_H)
    order, lists, cur, seen = [], [], [], set()

    def await_all(keys):
        for key in keys:
            if key not in seen:
                seen.add(key)
                cur.append(('wait', key))

    for op in prog:
        if op[0] == 'send':
            await_all(op[2])
            cur.append(('send', op[1]))
            continue
        s = sl[op[1]]
        ty, it, la, ex, hf = s
        if ty in ('mm', 'mq', 'h', 'wgu', 'wd'):
            await_all([('P%d' % k, it) for k in QUAD])
        if ty == 'h':
            await_all([('Q%d' % k, it) for k in PAIRED])
            await_all([('H', la, hf)])
            if la == 1 and ex == 0:
                cur.append(('drain', ('R', 0, hf)))
        if ty == 'mq':
            await_all([('T', 0, q) for q in PAIRED])
        if ty == 'nr':
            await_all([('S', 0, ex)])
        if ty == 'mm' and la == 0:
            await_all([('O', 0, hf)])
        if ty == 'mm' and la == 1 and ex == 0:
            cur.append(('drain', ('O', 0, hf)))
        if ty == 'fin':
            await_all([('R', la, hf)])
        order.append(s)
        lists.append(cur)
        cur = []
    assert not cur and all(k in seen for k, _ in KEYS)
    return order, lists


def copy_keys():
    keys = []
    for i, f in enumerate(ITEMS):
        px, py, dx, dy, pn = FLOW[f]
        rows = {'X': px, 'Y': py, 'P0': BLK, 'DX': dx, 'DY': dy, 'ZX': BLK - px, 'ZY': BLK - py, 'ZD': BLK - dx - dy, 'P1': BLK, 'P2': BLK, 'P3': BLK}
        if pn:
            rows.update({'N': pn, 'ZN': BLK - pn, 'Q0': BLK, 'Q1': BLK})
        keys += [((k, i), r) for k, r in rows.items() if r]
    for s in PAIRED:
        keys += [(('T', 0, s), BLK), (('S', 0, s), 0), (('O', 0, s), BLK)]
    for la in PAIRED:
        for s in PAIRED:
            keys += [(('H', la, s), BLK), (('R', la, s), 0)]
    return keys


KEYS = copy_keys()
SID = {k: n for n, (k, _) in enumerate(KEYS)}
KROWS = dict(KEYS)
H_ITEMS = [i for i, f in enumerate(ITEMS) if FLOW[f][4]]
ATTN0 = (0, 4 + N_H[0])
W_ITEM = 8 + N_H[0] + N_H[1]


def shared_col(n, side, j):
    return 4096 * (n // 2) + 2048 * side + 1024 * (n % 2) + BLK * j


def head(h):
    return slice(h * HEAD_DIM, (h + 1) * HEAD_DIM)


def tile(n):
    return slice(n * TILE, (n + 1) * TILE)


def seq(s):
    return pl.ds(pl.multiple_of(s * SEQ, SEQ), SEQ)


def loop(n, body):
    lax.fori_loop(0, n, body, 0)


def rope_tables():
    pos = np.arange(SEQ, dtype=np.float64)
    inv = THETA ** (-2.0 * np.arange(HEAD_DIM // 2, dtype=np.float64) / HEAD_DIM)
    ang = pos[:, None] * inv[None, :]
    cos, sin = np.cos(ang), np.sin(ang)
    return (np.concatenate([cos, cos], 1).astype(np.float32), np.concatenate([-sin, sin], 1).astype(np.float32))


def width(key):
    narrow = key[0] == 'O' or (len(key) == 2 and ITEMS[key[1]] == 'Q')
    return HALF if narrow else D


def kernel(x_hbm, cos_ref, sin_ref, gq, gk, ga, gm, wq, wk, wv, wo, wg, wu, wd, out_hbm, full, full_n, act, h2, mj, acc, rs, xo, st_out, st_in, wt, gains, gain_in, gain_ref, send_sem, recv_sem, wt_sem, gs_sem, gr_sem, io_sem, gi_sem):
    zz = lax.axis_index('dp')
    me = lax.axis_index('fsdp')
    cc = me % 2
    xx = (me // 2) % 2
    yy = me // 4

    def at(y, x, c):
        return y * 4 + x * 2 + c

    f_p = at(yy, xx, 1 - cc)
    f_x = at(yy, 1 - xx, cc)
    f_y = at(1 - yy, xx, cc)
    f_d = at(1 - yy, 1 - xx, cc)
    n_me, n_y = yy * 2 + cc, (1 - yy) * 2 + cc
    dev_p, dev_x, dev_y, dev_z = (zz, f_p), (zz, f_x), (zz, f_y), (1 - zz, me)

    x_copy = pltpu.make_async_copy(x_hbm, act.at[0], io_sem)
    x_copy.start()

    gain_loads = [pltpu.make_async_copy(g, gain_in.at[k], gi_sem.at[k]) for k, g in enumerate((gq, gk, ga, gm))]
    for cp in gain_loads:
        cp.start()
    for k, cp in enumerate(gain_loads):
        cp.wait()
        for la in PAIRED:
            gain_ref[la * 4 + k:la * 4 + k + 1, :] = gain_in[k, la:la + 1, :].astype(jnp.float32)

    barrier = pltpu.get_barrier_semaphore()
    for k in range(1, N_BLK):
        pl.semaphore_signal(barrier, inc=1, device_id=(zz, (me + k) % N_BLK), device_id_type=MESH)
    pl.semaphore_signal(barrier, inc=1, device_id=dev_z, device_id_type=MESH)
    pl.semaphore_wait(barrier, N_BLK)

    def m16(v):
        return pl.multiple_of(v, 16)

    def m256(v):
        return pl.multiple_of(v, 256)

    def remote(key, src, dst, dev):
        return pltpu.make_async_remote_copy(src, dst, send_sem.at[SID[key]], recv_sem.at[SID[key]], device_id=dev, device_id_type=MESH)

    def same_size(key):
        if key[0] == 'R':
            piece = rs.at[0, 0]
        elif key[0] == 'S':
            piece = st_in.at[key[2]]
        else:
            piece = full.at[0, 0, pl.ds(0, KROWS[key]), pl.ds(0, width(key))]
        return remote(key, piece, piece, dev_p)

    def arrived(key):
        same_size(key).wait_recv()

    def own_pieces(i, side):
        la = int(i >= ATTN0[1])
        if i >= W_ITEM:
            if i == W_ITEM + 2:
                return [(wd.at[la, pl.ds(3 * BLK, BLK), :], 0, D)]
            cols = [1024 * (4 * (i - W_ITEM) + n) + 3 * BLK for n in QUAD]
        elif i in H_ITEMS:
            j = i - ATTN0[la] - 4
            cols = [m256(shared_col(n, side, j)) for n in QUAD]
        elif ITEMS[i] == 'Q':
            return [((wq, wk, wv)[i].at[0, :, pl.ds(m256(HALF * side), HALF)], 0, HALF)]
        else:
            return [((wq, wk, wv, wo)[i - ATTN0[la]].at[la], 0, D)]
        out = []
        for n, c in enumerate(cols):
            out.append((wg.at[la, :, pl.ds(c, BLK)], n * TILE, BLK))
            out.append((wu.at[la, :, pl.ds(c, BLK)], n * TILE + BLK, BLK))
        return out

    def send_own(key, side, off, dev):
        i = key[1]
        part = pl.ds(off, KROWS[key])
        for src, c0, nc in own_pieces(i, side):
            remote(key, src.at[part, :], full.at[i, me, part, pl.ds(c0, nc)], dev).start()

    def push(key, blk, off, dev):
        piece = full.at[key[1], blk, pl.ds(off, KROWS[key]), pl.ds(0, width(key))]
        remote(key, piece, piece, dev).start()

    def push_n(key, off, dev):
        piece = full_n.at[H_ITEMS.index(key[1]), n_y, pl.ds(off, KROWS[key]), :]
        remote(key, piece, piece, dev).start()

    def own_n(key, off, dev):
        i = key[1]
        la = int(i >= ATTN0[1])
        r0 = BLK * (i - ATTN0[la] - 4)
        rr = KROWS[key]
        remote(key, wd.at[la, pl.ds(m16(r0 + off), rr), :], full_n.at[H_ITEMS.index(i), n_me, pl.ds(off, rr), :], dev).start()

    def transfer(op):
        key = op[1]
        if op[0] == 'wait':
            return arrived(key)
        if op[0] == 'drain':
            return same_size(key).wait_send()
        kind = key[0]
        if kind == 'T':
            return remote(key, x_hbm.at[pl.ds(key[2] * SEQ, SEQ), :], xo.at[key[2]], dev_x).start()
        if kind == 'S':
            return remote(key, st_out.at[key[2]], st_in.at[key[2]], dev_x).start()
        if kind == 'O':
            sq = pl.ds(key[2] * SEQ, SEQ)
            return remote(key, act.at[1, sq, pl.ds(HALF, HALF)], act.at[4, sq, pl.ds(m256(HALF * xx), HALF)], dev_x).start()
        if kind == 'H':
            la, s = key[1:]
            return remote(key, h2.at[la, s, pl.ds(0, SEQ), :], h2.at[la, s, pl.ds(SEQ, SEQ), :], dev_x).start()
        if kind == 'R':
            la, s = key[1:]
            return remote(key, acc.at[s, pl.ds(SEQ, SEQ), :], rs.at[la, s], dev_x).start()
        px, py, dx, dy, pn = FLOW[ITEMS[key[1]]]
        off_d = m16((BLK - dx - dy) * zz)
        steps = {
            'X': lambda: send_own(key, 1 - xx, m16((BLK - px) * zz), dev_x),
            'Y': lambda: send_own(key, xx, m16((BLK - py) * zz), dev_y),
            'P0': lambda: send_own(key, xx, 0, dev_p),
            'ZX': lambda: push(key, f_x, m16(px * zz), dev_z),
            'ZY': lambda: push(key, f_y, m16(py * zz), dev_z),
            'ZD': lambda: push(key, f_d, m16((dx + dy) * zz), dev_z),
            'DX': lambda: push(key, f_y, off_d, dev_x),
            'DY': lambda: push(key, f_x, m16(off_d + dx), dev_y),
            'P1': lambda: push(key, f_x, 0, dev_p),
            'P2': lambda: push(key, f_y, 0, dev_p),
            'P3': lambda: push(key, f_d, 0, dev_p),
            'N': lambda: own_n(key, m16((BLK - pn) * zz), dev_y),
            'Q0': lambda: own_n(key, 0, dev_p),
            'ZN': lambda: push_n(key, m16(pn * zz), dev_z),
            'Q1': lambda: push_n(key, 0, dev_p),
        }
        steps[kind]()

    order, lists = plan()
    n_slot = len(order)

    def load(parts, slot):
        for src, dst in parts:
            pltpu.make_async_copy(src, dst, wt_sem.at[slot]).start()

    def others(i, n):
        slot = n % SLOTS
        cols = pl.ds(n * TILE, TILE)
        load([(full.at[i, (me + k) % N_BLK, :, cols], wt.at[slot, (me + k) % N_BLK]) for k in range(1, N_BLK)], slot)

    def wait_tile(n, blocks=N_BLK):
        slot = n % SLOTS
        part = wt.at[slot, pl.ds(0, blocks)]
        pltpu.make_async_copy(full.at[0, pl.ds(0, blocks), :, pl.ds(0, TILE)], part, wt_sem.at[slot]).wait()

    def load_mm(i, la, role, n):
        slot = n % SLOTS
        cols = pl.ds(n * TILE, TILE)
        for k, w in enumerate((wq, wk, wv, wo)):
            pl.when(role == k)(functools.partial(load, [(w.at[la, :, cols], wt.at[slot, me])], slot))
        pl.when(role == 4)(functools.partial(load, [(wd.at[1, pl.ds(3 * BLK, BLK), cols], wt.at[slot, me])], slot))
        others(i, n)

    def load_gu(i, la, col, n):
        slot = n % SLOTS
        c = pl.ds(m256(col(n)), BLK)
        load([(wg.at[la, :, c], wt.at[slot, me, :, pl.ds(0, BLK)]), (wu.at[la, :, c], wt.at[slot, me, :, pl.ds(BLK, BLK)])], slot)
        others(i, n)

    def load_dn(hn, la, j, n):
        slot = n % SLOTS
        cols = pl.ds(n * TILE, TILE)
        parts = [(wd.at[la, pl.ds(m256(j * BLK), BLK), cols], wt.at[slot, n_me])]
        parts += [(full_n.at[hn, (n_me + k) % 4, :, cols], wt.at[slot, (n_me + k) % 4]) for k in range(1, 4)]
        load(parts, slot)

    def gain_row(la, k):
        return jnp.concatenate([gains[f, pl.ds(la * 4 + k, 1), :] for f in range(N_BLK)], axis=1)

    def scaled(v, gain):
        a = v.astype(jnp.bfloat16).astype(jnp.float32)
        ms = jnp.mean(a * a, axis=-1, keepdims=True)
        return a * lax.rsqrt(ms + EPS) * gain

    def rows(body):
        def step(r, carry):
            body(pl.multiple_of(r * RB, RB))
            return carry

        loop(SEQ // RB, step)

    def act_rows(s, r0):
        return pl.ds(pl.multiple_of(s * SEQ + r0, RB), RB)

    def norm_rope(la, k, dst, s):
        gain = gain_row(la, k)

        def body(r0):
            v = scaled(acc[s, pl.ds(r0, RB), :], gain)
            c = cos_ref[pl.ds(r0, RB), :]
            sn = sin_ref[pl.ds(r0, RB), :]
            for h in range(D // HEAD_DIM):
                part = v[:, head(h)]
                turned = pltpu.roll(part, HEAD_DIM // 2, 1)
                act[dst, act_rows(s, r0), head(h)] = (part * c + turned * sn).astype(jnp.bfloat16)

        rows(body)

    def attention(q8, la, s):
        split = (la == 0) & (q8 == 0)
        dst = jnp.where(split, 4, 1)
        base = jnp.where(split, xx * (HALF), q8 * (HALF))
        row = lax.broadcasted_iota(jnp.int32, (SEQ, SEQ), 0)
        col = lax.broadcasted_iota(jnp.int32, (SEQ, SEQ), 1)
        causal = row >= col
        sq = seq(s)

        def step(h, carry):
            for u in PAIRED:
                lanes = pl.ds(pl.multiple_of((q8 * 8 + h * 2 + u) * HEAD_DIM, HEAD_DIM), HEAD_DIM)
                q, k, v = act[1, sq, lanes], act[2, sq, lanes], act[3, sq, lanes]
                sc = lax.dot_general(q, k, (((1,), (1,)), ((), ())), preferred_element_type=jnp.float32) * (HEAD_DIM ** -0.5)
                sc = jnp.where(causal, sc, -jnp.inf)
                e = jnp.exp(sc - jnp.max(sc, axis=-1, keepdims=True))
                p = (e / jnp.sum(e, axis=-1, keepdims=True)).astype(jnp.bfloat16)
                out = pl.ds(pl.multiple_of(base + (h * 2 + u) * HEAD_DIM, HEAD_DIM), HEAD_DIM)
                act[dst, sq, out] = jnp.dot(p, v, preferred_element_type=jnp.float32).astype(jnp.bfloat16)
            return carry

        loop(4, step)

    def mm(i, la, role, hf):
        s0 = jnp.where(hf == 2, 0, hf)
        s1 = jnp.where(hf == 2, 2, hf + 1)
        lhs = jnp.where(role < 3, 0, jnp.where((role == 3) & (la == 1), 1, 4))
        load_mm(i, la, role, 0)
        for n in range(N_TILE):
            if n + 1 < N_TILE:
                load_mm(i, la, role, n + 1)
            wait_tile(n)
            cols = tile(n)

            def one(s, carry):
                left = act[lhs, seq(s), :]
                prod = jnp.dot(left, wt[n % SLOTS].reshape(D, TILE), preferred_element_type=jnp.float32)
                acc[s, :SEQ, cols] = jnp.where(role == 4, acc[s, :SEQ, cols], 0.0) + prod
                return carry

            lax.fori_loop(s0, s1, one, 0)

        def epilogue(s, carry):
            @pl.when(role == 0)
            def _():
                norm_rope(la, 0, 1, s)

            @pl.when(role == 1)
            def _():
                norm_rope(la, 1, 2, s)

            @pl.when(role == 2)
            def _():
                def body(r0):
                    act[3, act_rows(s, r0), :] = acc[s, pl.ds(r0, RB), :].astype(jnp.bfloat16)

                rows(body)

            @pl.when(role == 3)
            def _():
                gain = gain_row(la, 2)

                def body(r0):
                    h = act[0, act_rows(s, r0), :].astype(jnp.float32) + scaled(acc[s, pl.ds(r0, RB), :], gain)
                    h2[la, s, pl.ds(r0, RB), :] = h.astype(jnp.bfloat16)

                rows(body)

            return carry

        lax.fori_loop(s0, s1, epilogue, 0)

    def load_mq(k, n):
        slot = n % SLOTS
        for r, w in enumerate((wq, wk, wv)):
            own = w.at[0, :, pl.ds(m256(HALF * xx + n * TILE), TILE)]
            pl.when(k == r)(functools.partial(load, [(own, wt.at[slot, me])], slot))
        others(k, n)

    def shared_qkv(k):
        load_mq(k, 0)
        for n in PAIRED:
            if n == 0:
                load_mq(k, 1)
            wait_tile(n)
            cols = tile(n)

            def one(s, carry):
                w = wt[n % SLOTS].reshape(D, TILE)
                sq = seq(s)
                acc[s, :SEQ, cols] = jnp.dot(act[0, sq, :], w, preferred_element_type=jnp.float32)
                acc[s, SEQ:, cols] = jnp.dot(xo[s], w, preferred_element_type=jnp.float32)
                return carry

            loop(2, one)

        @pl.when(k == 2)
        def _():
            def keep(s, carry):
                for part in PAIRED:
                    def body(r0, part=part):
                        v = acc[s, pl.ds(part * SEQ + r0, RB), :HALF]
                        act[3, act_rows(s, r0), part * (HALF):(part + 1) * (HALF)] = v.astype(jnp.bfloat16)

                    rows(body)
                return carry

            loop(2, keep)

        @pl.when(k < 2)
        def _():
            def squares(s, carry):
                for part in PAIRED:
                    for r in PAIRED:
                        r0 = part * SEQ + r * HEAD_DIM
                        total = jnp.zeros((HEAD_DIM, HEAD_DIM), jnp.float32)
                        for h in range(8):
                            a = acc[s, r0:r0 + HEAD_DIM, head(h)].astype(jnp.bfloat16).astype(jnp.float32)
                            total = total + a * a
                        col = jnp.broadcast_to(jnp.sum(total, axis=-1, keepdims=True), (HEAD_DIM, HEAD_DIM))
                        st_out[k, s * 2 + part, :, head(r)] = col.T[:8, :]
                return carry

            loop(2, squares)

    def shared_rope(k):
        gain = jnp.concatenate([gains[xx * 4 + f, pl.ds(k, 1), :] for f in QUAD], axis=1)

        def one(s, carry):
            for part in PAIRED:
                for r in PAIRED:
                    lanes = head(r)
                    sums = st_out[k, s * 2 + part, :, lanes] + st_in[k, s * 2 + 1 - part, :, lanes]
                    col = jnp.broadcast_to(sums[:1, :], (HEAD_DIM, HEAD_DIM)).T
                    inv = lax.rsqrt(col * (1.0 / D) + EPS)
                    c, sn = cos_ref[lanes, :], sin_ref[lanes, :]
                    r0 = part * SEQ + r * HEAD_DIM
                    rr = pl.ds(pl.multiple_of(s * SEQ + r * HEAD_DIM, HEAD_DIM), HEAD_DIM)
                    for h in range(8):
                        hs = head(h)
                        a = acc[s, r0:r0 + HEAD_DIM, hs].astype(jnp.bfloat16).astype(jnp.float32)
                        v = a * inv * gain[:, hs]
                        turned = pltpu.roll(v, HEAD_DIM // 2, 1)
                        o0 = part * (HALF) + h * HEAD_DIM
                        act[k + 1, rr, o0:o0 + HEAD_DIM] = (v * c + turned * sn).astype(jnp.bfloat16)
            return carry

        loop(2, one)

    def swiglu(prod):
        gate = prod[:, :BLK].astype(jnp.bfloat16).astype(jnp.float32)
        up = prod[:, BLK:].astype(jnp.bfloat16).astype(jnp.float32)
        return (jax.nn.silu(gate) * up).astype(jnp.bfloat16)

    def shared_mlp(i, hn, la, j, s):
        def col(n):
            return shared_col(n, xx, j)

        load_gu(i, la, col, 0)
        for n in range(N_TILE):
            if n + 1 < N_TILE:
                load_gu(i, la, col, n + 1)
            else:
                load_dn(hn, la, j, 0)
            wait_tile(n)
            prod = jnp.dot(h2[la, s], wt[n % SLOTS].reshape(D, TILE), preferred_element_type=jnp.float32)
            mj[:, n * BLK:(n + 1) * BLK] = swiglu(prod)
        for n in range(N_TILE):
            if n + 1 < N_TILE:
                load_dn(hn, la, j, n + 1)
            wait_tile(n, 4)
            cols = tile(n)
            prod = jnp.dot(mj[...], wt[n % SLOTS, :4].reshape(4 * BLK, TILE), preferred_element_type=jnp.float32)
            acc[s, :, cols] = jnp.where(j > 0, acc[s, :, cols], 0.0) + prod

    def plain_gu(i, e):
        def col(n):
            return 1024 * (4 * e + n) + 3 * BLK

        load_gu(i, 1, col, 0)
        for n in range(N_TILE):
            if n + 1 < N_TILE:
                load_gu(i, 1, col, n + 1)
            wait_tile(n)

            def one(s, carry):
                prod = jnp.dot(h2[1, s, :SEQ], wt[n % SLOTS].reshape(D, TILE), preferred_element_type=jnp.float32)
                act[4, seq(s), pl.ds(m256(e * 1024 + n * BLK), BLK)] = swiglu(prod)
                return carry

            loop(2, one)

    def finish(la, s):
        gain = gain_row(la, 3)

        def body(r0):
            y = scaled(acc[s, pl.ds(r0, RB), :] + rs[la, s, pl.ds(r0, RB), :], gain)
            act[0, act_rows(s, r0), :] = (h2[la, s, pl.ds(r0, RB), :].astype(jnp.float32) + y).astype(jnp.bfloat16)

        rows(body)

    def pick(p, values):
        out = jnp.int32(0)
        for k, v in enumerate(values):
            if v:
                out = jnp.where(p == k, v, out)
        return out

    gain_copies = []
    for k in range(1, N_BLK):
        cp = pltpu.make_async_remote_copy(gain_ref, gains.at[me], gs_sem.at[k], gr_sem.at[k], device_id=(zz, (me + k) % N_BLK), device_id_type=MESH)
        gain_copies.append(cp)

    types = ['mm', 'at', 'h', 'wgu', 'wd', 'fin', 'mq', 'nr']

    def step(p, carry):
        for k in range(n_slot):
            if not lists[k]:
                continue

            @pl.when(p == k)
            def _(k=k):
                if k == 0:
                    for cp in gain_copies:
                        cp.start()
                for op in lists[k]:
                    transfer(op)
                if k == 0:
                    x_copy.wait()
                    for cp in gain_copies:
                        cp.wait()
                    gains[pl.ds(me, 1)] = gain_ref[...][None]

        ty = pick(p, [types.index(o[0]) for o in order])
        item = pick(p, [o[1] for o in order])
        la = pick(p, [o[2] for o in order])
        ex = pick(p, [o[3] for o in order])
        hf = pick(p, [o[4] for o in order])
        hn = pick(p, [H_ITEMS.index(o[1]) if o[0] == 'h' else 0 for o in order])
        pl.when((ty == 0) | (ty == 4))(lambda: mm(item, la, ex, hf))
        pl.when(ty == 1)(lambda: attention(ex, la, hf))
        pl.when(ty == 2)(lambda: shared_mlp(item, hn, la, ex, hf))
        pl.when(ty == 3)(lambda: plain_gu(item, ex))
        pl.when(ty == 5)(lambda: finish(la, hf))
        pl.when(ty == 6)(lambda: shared_qkv(ex))
        pl.when(ty == 7)(lambda: shared_rope(ex))
        return carry

    loop(n_slot, step)

    out_copy = pltpu.make_async_copy(act.at[0], out_hbm, io_sem)
    out_copy.start()
    drained = [op[1] for ops in lists for op in ops if op[0] == 'drain']
    for key, _ in KEYS:
        if key not in drained:
            same_size(key).wait_send()
    out_copy.wait()


def solution(mesh):
    cos_np, sin_np = rope_tables()
    hbm = pl.BlockSpec(memory_space=pl.ANY)
    vmem = pl.BlockSpec(memory_space=pltpu.VMEM)
    n_copy = len(KEYS)

    def local_fn(tokens, weights, gain_vecs):
        flat = tokens.reshape(ROWS, D)
        out = pl.pallas_call(
            kernel,
            out_shape=(
                jax.ShapeDtypeStruct((ROWS, D), jnp.bfloat16),
                jax.ShapeDtypeStruct((len(ITEMS), N_BLK, BLK, D), jnp.bfloat16),
                jax.ShapeDtypeStruct((len(H_ITEMS), 4, BLK, D), jnp.bfloat16),
            ),
            in_specs=[hbm, vmem, vmem] + [hbm] * 11,
            out_specs=(hbm, hbm, hbm),
            scratch_shapes=[
                pltpu.VMEM((5, ROWS, D), jnp.bfloat16),
                pltpu.VMEM((2, 2, 2 * SEQ, D), jnp.bfloat16),
                pltpu.VMEM((2 * SEQ, 4 * BLK), jnp.bfloat16),
                pltpu.VMEM((2, 2 * SEQ, D), jnp.float32),
                pltpu.VMEM((2, 2, SEQ, D), jnp.float32),
                pltpu.VMEM((2, SEQ, D), jnp.bfloat16),
                pltpu.VMEM((2, 4, 8, SEQ), jnp.float32),
                pltpu.VMEM((2, 4, 8, SEQ), jnp.float32),
                pltpu.VMEM((2, N_BLK, BLK, TILE), jnp.bfloat16),
                pltpu.VMEM((N_BLK, 8, BLK), jnp.float32),
                pltpu.VMEM((4, 2, BLK), jnp.bfloat16),
                pltpu.VMEM((8, BLK), jnp.float32),
                pltpu.SemaphoreType.DMA((n_copy,)),
                pltpu.SemaphoreType.DMA((n_copy,)),
                pltpu.SemaphoreType.DMA((2,)),
                pltpu.SemaphoreType.DMA((N_BLK,)),
                pltpu.SemaphoreType.DMA((N_BLK,)),
                pltpu.SemaphoreType.DMA,
                pltpu.SemaphoreType.DMA((4,)),
            ],
            compiler_params=pltpu.CompilerParams(collective_id=0, has_side_effects=True, vmem_limit_bytes=60 * 1024 * 1024),
        )(flat, jnp.asarray(cos_np), jnp.asarray(sin_np), *gain_vecs, *weights)
        return out[0].reshape(tokens.shape)

    mapped = jax.shard_map(local_fn, mesh=mesh, in_specs=(P(('dp', 'fsdp')), P(None, 'fsdp'), P(None, 'fsdp')), out_specs=P(('dp', 'fsdp')), check_vma=False)

    def run(tokens, w_query, w_key, w_value, w_out, w_gate, w_up, w_down, g_query, g_key, g_attn, g_mlp):
        return mapped(tokens, (w_query, w_key, w_value, w_out, w_gate, w_up, w_down), (g_query, g_key, g_attn, g_mlp))

    return run
```
